32 devices in a mesh: rep: 2 (over x), dp: 16 (over y, z, core).
Axes of the slice: x: 2, y: 2, z: 4, core: 2. Of those that a mesh axis runs over, the one named last changes fastest.
Arguments:
- x: bfloat16 [32, 2048, 1024], P(('rep', 'dp')), parts along dimension 0
- dy: bfloat16 [32, 2048, 1024], P(('rep', 'dp')), parts along dimension 0
- w_gate: bfloat16 [2, 1024, 3200], replicated
- w_up: bfloat16 [2, 1024, 3200], replicated
- w_down: bfloat16 [2, 3200, 1024], replicated
- m_w_gate: float32 [2, 1024, 3200], P(None, 'dp')
- m_w_up: float32 [2, 1024, 3200], P(None, 'dp')
- m_w_down: float32 [2, 3200, 1024], P(None, 'dp')
- v_w_gate: float32 [2, 1024, 3200], P(None, 'dp')
- v_w_up: float32 [2, 1024, 3200], P(None, 'dp')
- v_w_down: float32 [2, 3200, 1024], P(None, 'dp')
Outputs:
- output 1: bfloat16 [4, 1024, 3200], P('rep'), parts along dimension 0
- output 2: bfloat16 [4, 1024, 3200], P('rep'), parts along dimension 0
- output 3: bfloat16 [4, 3200, 1024], P('rep'), parts along dimension 0
- output 4: float32 [4, 1024, 3200], P('rep', 'dp'), parts along dimension 0
- output 5: float32 [4, 1024, 3200], P('rep', 'dp'), parts along dimension 0
- output 6: float32 [4, 3200, 1024], P('rep', 'dp'), parts along dimension 0
- output 7: float32 [4, 1024, 3200], P('rep', 'dp'), parts along dimension 0
- output 8: float32 [4, 1024, 3200], P('rep', 'dp'), parts along dimension 0
- output 9: float32 [4, 3200, 1024], P('rep', 'dp'), parts along dimension 0
There are 2 independent parts. The reference program is written for one: setup_inputs(seed, part) draws one part's arguments, and reference() takes and returns one part's arrays. A program takes and returns all parts, laid end to end along the dimension named above; an argument that names none is the same for every part.
All inputs are finite; a program needn't handle non-finite values.
Results may differ from the reference program's by a relative error of at most 0.022.
Values are sent between devices in bfloat16 or wider.
A program may use at most 2 GiB of HBM per device.

```python
import jax
import jax.numpy as jnp
from jax import lax

SEQUENCES = 16
TOKENS = 2048
D = 1024
FF = 3200
LAYERS = 2
NAMES = ("w_gate", "w_up", "w_down")
SHAPES = {"w_gate": (LAYERS, D, FF), "w_up": (LAYERS, D, FF), "w_down": (LAYERS, FF, D)}


def bump(key, n, height):
    away = (jnp.arange(n, dtype=jnp.int32) - jax.random.randint(key, (), 0, n, jnp.int32)) % n
    return jnp.where(away < n // 8, height, 1.0)


def together(key, own, strength):
    shared = jax.random.normal(key, own.shape[1:], jnp.float32)
    return (own + strength * shared) * lax.rsqrt(1 + strength * strength)


def setup_inputs(seed: int = 0, part: int = 0) -> dict:
    kx, kdy, ka, kb, kz, kf, kh, kl, *keys = jax.random.split(jax.random.key(seed), 8 + 3 * len(NAMES))
    kx, kdy, ka, kb = (jax.random.fold_in(k, part) for k in (kx, kdy, ka, kb))
    kw, km, kv = (keys[i::3] for i in range(3))
    shape = (SEQUENCES, TOKENS, D)
    much_x, much_dy = jax.random.uniform(kz, (2,), jnp.float32, 0.0, 1.0)
    loud = 2.0 ** jax.random.uniform(jax.random.fold_in(kz, 1), (), jnp.float32, -1.0, 2.0)
    layers = 2.0 ** jax.random.uniform(kl, (LAYERS, 1, 1), jnp.float32, -1.0, 1.0)
    x = together(ka, jax.random.normal(kx, shape, jnp.float32), much_x) * bump(kf, D, 4.0)
    dy = together(kb, jax.random.normal(kdy, shape, jnp.float32), much_dy)
    drawn = {"x": x.astype(jnp.bfloat16), "dy": (loud * dy * (SEQUENCES * TOKENS) ** -0.5).astype(jnp.bfloat16)}
    for key, name in zip(kw, NAMES, strict=True):
        w = jax.random.normal(key, SHAPES[name], jnp.float32) * SHAPES[name][1] ** -0.5
        drawn[name] = (w * {"w_gate": 1.0, "w_up": bump(kh, FF, 4.0), "w_down": layers}[name]).astype(jnp.bfloat16)
    for key, name in zip(km, NAMES, strict=True):
        drawn[f"m_{name}"] = 0.1 * jax.random.normal(key, SHAPES[name], jnp.float32)
    for key, name in zip(kv, NAMES, strict=True):
        drawn[f"v_{name}"] = jax.random.uniform(key, SHAPES[name], jnp.float32, 0.005, 0.015)
    return drawn


def matmul(a, w):
    return jnp.dot(a, w, preferred_element_type=jnp.float32).astype(jnp.bfloat16)


def normed(h):
    wide = h.astype(jnp.float32)
    scale = lax.rsqrt(jnp.mean(wide**2, -1, keepdims=True) + 1e-6)
    return (wide * scale).astype(jnp.bfloat16)


def layer(h, w):
    a = normed(h)
    gate = jnp.dot(a, w["w_gate"], preferred_element_type=jnp.float32)
    up = jnp.dot(a, w["w_up"], preferred_element_type=jnp.float32)
    return h + matmul((jax.nn.silu(gate) * up).astype(jnp.bfloat16), w["w_down"])


def adamw(w, m, v, g):
    m = 0.9 * m + 0.1 * g
    v = 0.95 * v + 0.05 * g * g
    step = m * lax.rsqrt(v + 1e-8) + 0.1 * w
    return (w - 0.02 * step).astype(jnp.bfloat16), m, v


def clipped(gradients, sum_of_squares, count):
    factor = jnp.minimum(1.0, 0.5 * lax.rsqrt(sum_of_squares / count + 1e-30))
    return [g * factor for g in gradients]


def stack(weights, h):
    return lax.scan(lambda h, w: (layer(h, w), None), h, weights)[0]


def reference(x, dy, w_gate, w_up, w_down, m_w_gate, m_w_up, m_w_down, v_w_gate, v_w_up, v_w_down):
    weights = dict(zip(NAMES, (w_gate, w_up, w_down), strict=True))

    def take(so_far, sequence):
        h, by_y = sequence
        _, back = jax.vjp(lambda w: stack(w, h), weights)
        return jax.tree.map(lambda total, term: total + term.astype(jnp.float32), so_far, back(by_y)[0]), None

    none_yet = {name: jnp.zeros(w.shape, jnp.float32) for name, w in weights.items()}
    by_weights, _ = lax.scan(take, none_yet, (x, dy))
    gradients = [by_weights[name].astype(jnp.bfloat16).astype(jnp.float32) for name in NAMES]
    gradients = clipped(gradients, sum(jnp.sum(g * g) for g in gradients), sum(g.size for g in gradients))
    new = [
        adamw(w.astype(jnp.float32), m, v, g)
        for w, m, v, g in zip((w_gate, w_up, w_down), (m_w_gate, m_w_up, m_w_down), (v_w_gate, v_w_up, v_w_down), gradients, strict=True)
    ]
    return tuple(one[which] for which in range(3) for one in new)
```

```python
import functools

import jax
import jax.numpy as jnp
from jax import lax
from jax.experimental import pallas as pl
from jax.experimental.pallas import tpu as pltpu
from jax.sharding import PartitionSpec as P

MESH = pl.DeviceIdType.MESH
HBM = pltpu.HBM
D, FF, T = 1024, 3200, 2048
bf16, f32 = jnp.bfloat16, jnp.float32
SLOTS = 3


def place():
    me = lax.axis_index("dp")
    return lax.axis_index("rep"), me // 8, lax.rem(me // 2, 4), lax.rem(me, 2)


def device(r, y, z, c):
    return (r, y * 8 + z * 2 + c)


def greet(r, y, z, c):
    bar = pltpu.get_barrier_semaphore()
    peers = [device(r, y, z, 1 - c), device(r, 1 - y, z, c)] + [device(r, y, lax.rem(z + o, 4), c) for o in (1, 2, 3)]
    for p in peers:
        pl.semaphore_signal(bar, 1, device_id=p, device_id_type=MESH)
    pl.semaphore_wait(bar, len(peers))


class Reducer:
    def __init__(self, source, out, sums, rows, cols, total, bufs):
        self.source, self.out, self.sums = source, out, sums
        self.rows, self.cols, self.total = rows, cols, total
        (self.xr, self.xo, self.ys, self.yr, self.s1, self.zs, self.zr, self.go,
         self.xss, self.xrs, self.xls, self.yss, self.yrs, self.zss, self.zrs, self.gos, self.cx, self.cy, self.cz) = bufs
        self.r, self.y, self.z, self.c = place()

    @staticmethod
    def scratch(rows, cols, s=SLOTS):
        V, dma, reg = pltpu.VMEM, pltpu.SemaphoreType.DMA, pltpu.SemaphoreType.REGULAR
        return [
            V((s, 8, rows, cols), bf16), V((s, 8, rows, cols), bf16), V((s, 4, rows, cols), bf16), V((s, 4, rows, cols), bf16),
            V((s, 4, rows, cols), f32), V((s, 3, rows, cols), bf16), V((s, 3, rows, cols), bf16), V((s, rows, cols), bf16),
            dma((s,)), dma((s,)), dma((s,)), dma((s,)), dma((s,)), dma((s, 3)), dma((s, 3)), dma((s,)), reg, reg, reg((3,)),
        ]

    def copies_x(self, q):
        s = lax.rem(q, SLOTS)
        go = pltpu.make_async_remote_copy(
            self.source(q, 1 - self.c), self.xr.at[s], self.xss.at[s], self.xrs.at[s],
            device_id=device(self.r, self.y, self.z, 1 - self.c), device_id_type=MESH)
        own = pltpu.make_async_copy(self.source(q, self.c), self.xo.at[s], self.xls.at[s])
        return go, own

    def copy_y(self, q):
        s = lax.rem(q, SLOTS)
        return pltpu.make_async_remote_copy(
            self.ys.at[s], self.yr.at[s], self.yss.at[s], self.yrs.at[s],
            device_id=device(self.r, 1 - self.y, self.z, self.c), device_id_type=MESH)

    def copy_z(self, q, o):
        s = lax.rem(q, SLOTS)
        return pltpu.make_async_remote_copy(
            self.zs.at[s, o - 1], self.zr.at[s, 3 - o], self.zss.at[s, o - 1], self.zrs.at[s, 3 - o],
            device_id=device(self.r, self.y, lax.rem(self.z + o, 4), self.c), device_id_type=MESH)

    def copy_out(self, q):
        s = lax.rem(q, SLOTS)
        return pltpu.make_async_copy(self.go.at[s], self.out(q), self.gos.at[s])

    def signal(self, sem, dev):
        pl.semaphore_signal(sem, 1, device_id=dev, device_id_type=MESH)

    def stage0(self, q):
        @pl.when(q >= SLOTS)
        def _():
            pl.semaphore_wait(self.cx, 1)

        for copy in self.copies_x(q):
            copy.start()

    def stage1(self, q):
        s = lax.rem(q, SLOTS)
        go, own = self.copies_x(q)
        own.wait()
        go.wait()

        def add(i, _):
            b = (1 - self.y) * 4 + i
            self.ys[s, i] = (self.xo[s, b].astype(f32) + self.xr[s, b].astype(f32)).astype(bf16)
            b = self.y * 4 + i
            self.s1[s, i] = self.xo[s, b].astype(f32) + self.xr[s, b].astype(f32)
            return 0

        lax.fori_loop(0, 4, add, 0)

        @pl.when(q + SLOTS < self.total)
        def _():
            self.signal(self.cx, device(self.r, self.y, self.z, 1 - self.c))

        @pl.when(q >= SLOTS)
        def _():
            pl.semaphore_wait(self.cy, 1)

        self.copy_y(q).start()

    def stage2(self, q):
        s = lax.rem(q, SLOTS)
        self.copy_y(q).wait()
        for o in (1, 2, 3):
            b = lax.rem(self.z + o, 4)
            self.zs[s, o - 1] = (self.s1[s, b] + self.yr[s, b].astype(f32)).astype(bf16)
        self.s1[s, self.z] = self.s1[s, self.z] + self.yr[s, self.z].astype(f32)

        @pl.when(q + SLOTS < self.total)
        def _():
            self.signal(self.cy, device(self.r, 1 - self.y, self.z, self.c))

        for o in (1, 2, 3):

            @pl.when(q >= SLOTS)
            def _():
                pl.semaphore_wait(self.cz.at[o - 1], 1)

            self.copy_z(q, o).start()

    def stage3(self, q):
        s = lax.rem(q, SLOTS)

        @pl.when(q >= SLOTS)
        def _():
            self.copy_out(q - SLOTS).wait()

        for o in (1, 2, 3):
            self.copy_z(q, o).wait()
        total = self.s1[s, self.z] + self.zr[s, 0].astype(f32) + self.zr[s, 1].astype(f32) + self.zr[s, 2].astype(f32)
        total = total.astype(bf16)
        self.go[s] = total
        total = total.astype(f32)
        self.sums[...] += jnp.sum((total * total).reshape(-1, 8, self.cols), 0).reshape(8, -1, 128).sum(1)

        @pl.when(q + SLOTS < self.total)
        def _():
            for o in (1, 2, 3):
                self.signal(self.cz.at[3 - o], device(self.r, self.y, lax.rem(self.z + o, 4), self.c))

        self.copy_out(q).start()

    def tick(self, t, lags=(0, 1, 2, 3)):
        for lag, stage in reversed(list(zip(lags, (self.stage0, self.stage1, self.stage2, self.stage3)))):
            q = t - lag

            @pl.when((q >= 0) & (q < self.total))
            def _():
                stage(q)

    def finish(self):
        for i in range(SLOTS):
            self.copy_out(self.total - SLOTS + i).wait()


GC, GP = 640, 5
DC, DP = 256, 4


def scatter_kernel(dg_ref, dd_ref, g_out, d_out, sums_out, sums, *bufs):
    half = len(bufs) // 2
    r, y, z, c = place()
    greet(r, y, z, c)
    sums[...] = jnp.zeros_like(sums)

    def g_source(q, c):
        m, p = q // GP, lax.rem(q, GP)
        return dg_ref.at[m, :, c, :, pl.ds(pl.multiple_of(p * GC, 128), GC)]

    def g_to(q):
        m, p = q // GP, lax.rem(q, GP)
        return g_out.at[m, :, pl.ds(pl.multiple_of(p * GC, 128), GC)]

    def d_source(q, c):
        m, p = q // DP, lax.rem(q, DP)
        return dd_ref.at[m, :, c, :, pl.ds(pl.multiple_of(p * DC, 128), DC)]

    def d_to(q):
        m, p = q // DP, lax.rem(q, DP)
        return d_out.at[m, :, pl.ds(pl.multiple_of(p * DC, 128), DC)]

    gr = Reducer(g_source, g_to, sums, 64, GC, 4 * GP, bufs[:half])
    dr = Reducer(d_source, d_to, sums, 200, DC, 2 * DP, bufs[half:])
    lax.fori_loop(0, dr.total + 3, lambda t, _: (dr.tick(t), 0)[1], 0)
    dr.finish()
    lax.fori_loop(0, gr.total + 3, lambda t, _: (gr.tick(t), 0)[1], 0)
    gr.finish()
    sums_out[...] = sums[...]


def reduce_scatter(dg, dd):
    return pl.pallas_call(
        scatter_kernel,
        out_shape=(
            jax.ShapeDtypeStruct((4, 64, FF), bf16),
            jax.ShapeDtypeStruct((2, 200, D), bf16),
            jax.ShapeDtypeStruct((8, 128), f32),
        ),
        in_specs=[pl.BlockSpec(memory_space=HBM)] * 2,
        out_specs=(pl.BlockSpec(memory_space=HBM), pl.BlockSpec(memory_space=HBM), pl.BlockSpec(memory_space=pltpu.VMEM)),
        scratch_shapes=[pltpu.VMEM((8, 128), f32)] + Reducer.scratch(64, GC) + Reducer.scratch(200, DC),
        compiler_params=pltpu.CompilerParams(collective_id=0, has_side_effects=True, vmem_limit_bytes=60 * 2**20),
    )(dg.reshape(4, 8, 2, 64, FF), dd.reshape(2, 8, 2, 200, D))


def gather_kernel(sg, su, sd, og, ou, od, zs, zr, ys, yr, ds, dr, ls):
    r, y, z, c = place()
    greet(r, y, z, c)
    chunks = [(s, o, layer) for layer in range(2) for s, o in ((sg, og), (su, ou), (sd, od))]
    n = len(chunks)

    def block(y, z, c):
        return y * 8 + z * 2 + c

    def zat(o):
        return lax.rem(z + o, 4)

    partner, across = device(r, y, z, 1 - c), device(r, 1 - y, z, c)
    mine = block(y, z, c)
    sent = []

    def send(src, k, b, ssem, rsem, dev):
        _, o, layer = chunks[k]
        copy = pltpu.make_async_remote_copy(src, o.at[layer, b], ssem, rsem, device_id=dev, device_id_type=MESH)
        copy.start()
        sent.append(copy)

    def arrived(k, b, ssem, rsem, dev):
        _, o, layer = chunks[k]
        ref = o.at[layer, b]
        pltpu.make_async_remote_copy(ref, ref, ssem, rsem, device_id=dev, device_id_type=MESH).wait_recv()
        return ref

    local = []
    for k, (s, o, layer) in enumerate(chunks):
        for d in (1, 2, 3):
            send(s.at[layer], k, mine, zs.at[k, d - 1], zr.at[k, 3 - d], device(r, y, zat(d), c))
        send(s.at[layer], k, mine, ys.at[k, 0], yr.at[k, 0], across)
        send(s.at[layer], k, mine, ds.at[k, 0], dr.at[k, 0], partner)
        copy = pltpu.make_async_copy(s.at[layer], o.at[layer, mine], ls.at[k])
        copy.start()
        local.append(copy)
    for k in range(n + 1):
        if k < n:
            for d in (1, 2, 3):
                b = block(y, zat(d), c)
                ref = arrived(k, b, zs.at[k, d - 1], zr.at[k, d - 1], across)
                send(ref, k, b, ys.at[k, d], yr.at[k, d], across)
                send(ref, k, b, ds.at[k, d], dr.at[k, d], partner)
        if k >= 1:
            for d in range(4):
                b = block(1 - y, zat(d), c)
                ref = arrived(k - 1, b, ys.at[k - 1, d], yr.at[k - 1, d], across)
                send(ref, k - 1, b, ds.at[k - 1, 4 + d], dr.at[k - 1, 4 + d], partner)
    for k in range(n):
        for e in range(8):
            b = block(y if e < 4 else 1 - y, zat(e % 4), 1 - c)
            arrived(k, b, ds.at[k, e], dr.at[k, e], partner)
    for copy in sent:
        copy.wait_send()
    for copy in local:
        copy.wait()


def all_gather(sg, su, sd):
    dma = pltpu.SemaphoreType.DMA
    out = pl.pallas_call(
        gather_kernel,
        out_shape=(
            jax.ShapeDtypeStruct((2, 16, 64, FF), bf16),
            jax.ShapeDtypeStruct((2, 16, 64, FF), bf16),
            jax.ShapeDtypeStruct((2, 16, 200, D), bf16),
        ),
        in_specs=[pl.BlockSpec(memory_space=pltpu.VMEM)] * 3,
        out_specs=[pl.BlockSpec(memory_space=HBM)] * 3,
        scratch_shapes=[dma((6, 3)), dma((6, 3)), dma((6, 4)), dma((6, 4)), dma((6, 8)), dma((6, 8)), dma((6,))],
        compiler_params=pltpu.CompilerParams(collective_id=1, has_side_effects=True),
    )(sg, su, sd)
    return out[0].reshape(2, D, FF), out[1].reshape(2, D, FF), out[2].reshape(2, FF, D)


def dot(a, b, ca, cb):
    return lax.dot_general(a, b, (((ca,), (cb,)), ((), ())), preferred_element_type=f32)


def normed(h):
    wide = h.astype(f32)
    return (wide * lax.rsqrt(jnp.mean(wide**2, -1, keepdims=True) + 1e-6)).astype(bf16)


def normed_back(h, da):
    wide, da = h.astype(f32), da.astype(f32)
    scale = lax.rsqrt(jnp.mean(wide**2, -1, keepdims=True) + 1e-6)
    inner = jnp.mean(da * wide, -1, keepdims=True)
    return scale * da - wide * (scale**3 * inner)


def layer_back(a, gate, up, mid, wd, dh):
    dmid = dot(dh, wd, 1, 1).astype(bf16).astype(f32)
    sig = jax.nn.sigmoid(gate)
    silu = gate * sig
    dgate = (dmid * up * (sig + silu * (1 - sig))).astype(bf16)
    dup = (dmid * silu).astype(bf16)
    return dot(a, dgate, 0, 0).astype(bf16), dot(a, dup, 0, 0).astype(bf16), dot(mid, dh, 0, 0).astype(bf16), dgate, dup


def local_terms(x, dy, wg, wu, wd):
    h, kept = x, []
    for i in range(2):
        a = normed(h)
        gate, up = dot(a, wg[i], 1, 0), dot(a, wu[i], 1, 0)
        mid = (jax.nn.silu(gate) * up).astype(bf16)
        kept.append((h, a, gate, up, mid))
        if i == 0:
            h = h + dot(mid, wd[i], 1, 0).astype(bf16)
    h1, a1, gate1, up1, mid1 = kept[1]
    dwg1, dwu1, dwd1, dgate, dup = layer_back(a1, gate1, up1, mid1, wd[1], dy)
    da = dot(dgate, wg[1], 1, 1) + dot(dup, wu[1], 1, 1)
    dh = dy + normed_back(h1, da).astype(bf16)
    _, a0, gate0, up0, mid0 = kept[0]
    dwg0, dwu0, dwd0, _, _ = layer_back(a0, gate0, up0, mid0, wd[0], dh)
    return jnp.stack([dwg1, dwu1, dwg0, dwu0]), jnp.stack([dwd1, dwd0])


def adamw(w, m, v, g):
    m = 0.9 * m + 0.1 * g
    v = 0.95 * v + 0.05 * g * g
    step = m * lax.rsqrt(v + 1e-8) + 0.1 * w
    return (w - 0.02 * step).astype(bf16), m, v


def solution(mesh):
    def step(x, dy, wg, wu, wd, mg, mu, md, vg, vu, vd):
        dg, dd = local_terms(x[0], dy[0], wg, wu, wd)
        gg, gd, sums = reduce_scatter(dg, dd)
        squares = lax.psum(jnp.sum(sums), "dp")
        factor = jnp.minimum(1.0, 0.5 * lax.rsqrt(squares / (6 * D * FF) + 1e-30))
        me = lax.axis_index("dp")
        new = []
        for w, m, v, g in ((wg, mg, vg, gg[2::-2]), (wu, mu, vu, gg[3::-2]), (wd, md, vd, gd[::-1])):
            rows = m.shape[1]
            mine = lax.dynamic_slice_in_dim(w, me * rows, rows, 1)
            new.append(adamw(mine.astype(f32), m, v, g.astype(f32) * factor))
        weights = all_gather(*(n[0] for n in new))
        return (*weights, *(n[1] for n in new), *(n[2] for n in new))

    seq, rep, own = P(("rep", "dp")), P("rep"), P("rep", "dp")
    return jax.shard_map(
        step,
        mesh=mesh,
        in_specs=(seq, seq, P(), P(), P(), *[P(None, "dp")] * 6),
        out_specs=(rep,) * 3 + (own,) * 6,
        check_vma=False,
    )
```

```python
import functools

import jax
import jax.numpy as jnp
from jax import lax
from jax.experimental import pallas as pl
from jax.experimental.pallas import tpu as pltpu
from jax.sharding import PartitionSpec as P

MESH = pl.DeviceIdType.MESH
HBM = pltpu.HBM
D, FF, T = 1024, 3200, 2048
bf16, f32 = jnp.bfloat16, jnp.float32


def place():
    me = lax.axis_index("dp")
    return lax.axis_index("rep"), me // 8, lax.rem(me // 2, 4), lax.rem(me, 2)


def device(r, y, z, c):
    return (r, y * 8 + z * 2 + c)


def greet(r, y, z, c):
    bar = pltpu.get_barrier_semaphore()
    peers = [device(r, y, z, 1 - c), device(r, 1 - y, z, c)] + [device(r, y, lax.rem(z + o, 4), c) for o in (1, 2, 3)]
    for p in peers:
        pl.semaphore_signal(bar, 1, device_id=p, device_id_type=MESH)
    pl.semaphore_wait(bar, len(peers))


def dot(a, b, ca, cb):
    return lax.dot_general(a, b, (((ca,), (cb,)), ((), ())), preferred_element_type=f32)


class Reducer:
    LAGS = (0, 1, 3, 5)

    def __init__(self, source, own, out, sums, slots, total, bufs):
        self.source, self.own, self.out, self.sums, self.total = source, own, out, sums, total
        self.nx, self.ny, self.nz = slots
        (self.xr, self.ys, self.yr, self.s1, self.acc, self.zs, self.zr, self.go,
         self.xss, self.xrs, self.yss, self.yrs, self.zss, self.zrs, self.gos, self.cx, self.cy, self.cz) = bufs
        self.r, self.y, self.z, self.c = place()

    @staticmethod
    def scratch(shape, parts, slots):
        nx, ny, nz = slots
        V, dma, reg = pltpu.VMEM, pltpu.SemaphoreType.DMA, pltpu.SemaphoreType.REGULAR
        return [
            V((nx, 8, *shape), bf16), V((ny, 4, *shape), bf16), V((ny, 4, *shape), bf16), V((ny, 4, *shape), f32),
            V((nz, *shape), f32), V((nz, 3, *shape), bf16), V((nz, 3, *shape), bf16), V((nz, *shape), bf16),
            dma((nx, parts)), dma((nx, parts)), dma((ny,)), dma((ny,)), dma((nz, 3)), dma((nz, 3)), dma((nz,)), reg, reg, reg((3,)),
        ]

    def copies_x(self, q):
        s = lax.rem(q, self.nx)
        return [
            pltpu.make_async_remote_copy(
                src, self.xr.at[s] if b is None else self.xr.at[s, b], self.xss.at[s, b or 0], self.xrs.at[s, b or 0],
                device_id=device(self.r, self.y, self.z, 1 - self.c), device_id_type=MESH)
            for src, b in self.source(q, 1 - self.c)
        ]

    def copy_y(self, q):
        s = lax.rem(q, self.ny)
        return pltpu.make_async_remote_copy(
            self.ys.at[s], self.yr.at[s], self.yss.at[s], self.yrs.at[s],
            device_id=device(self.r, 1 - self.y, self.z, self.c), device_id_type=MESH)

    def copy_z(self, q, o):
        s = lax.rem(q, self.nz)
        return pltpu.make_async_remote_copy(
            self.zs.at[s, o - 1], self.zr.at[s, 3 - o], self.zss.at[s, o - 1], self.zrs.at[s, 3 - o],
            device_id=device(self.r, self.y, lax.rem(self.z + o, 4), self.c), device_id_type=MESH)

    def copy_out(self, q):
        s = lax.rem(q, self.nz)
        return pltpu.make_async_copy(self.go.at[s], self.out(q), self.gos.at[s])

    def signal(self, sem, dev):
        pl.semaphore_signal(sem, 1, device_id=dev, device_id_type=MESH)

    def stage0(self, q):
        @pl.when(q >= self.nx)
        def _():
            pl.semaphore_wait(self.cx, 1)

        for copy in self.copies_x(q):
            copy.start()
        self.own.start(q)

    def stage1(self, q):
        x, s = lax.rem(q, self.nx), lax.rem(q, self.ny)
        self.own.wait(q)
        for copy in self.copies_x(q):
            copy.wait()

        def add(i, _):
            b = (1 - self.y) * 4 + i
            self.ys[s, i] = (self.own.read(q, b).astype(f32) + self.xr[x, b].astype(f32)).astype(bf16)
            b = self.y * 4 + i
            self.s1[s, i] = self.own.read(q, b).astype(f32) + self.xr[x, b].astype(f32)
            return 0

        lax.fori_loop(0, 4, add, 0)

        @pl.when(q + self.nx < self.total)
        def _():
            self.signal(self.cx, device(self.r, self.y, self.z, 1 - self.c))

        @pl.when(q >= self.ny)
        def _():
            pl.semaphore_wait(self.cy, 1)

        self.copy_y(q).start()

    def stage2(self, q):
        s, t = lax.rem(q, self.ny), lax.rem(q, self.nz)
        self.copy_y(q).wait()
        for o in (1, 2, 3):
            b = lax.rem(self.z + o, 4)
            self.zs[t, o - 1] = (self.s1[s, b] + self.yr[s, b].astype(f32)).astype(bf16)
        self.acc[t] = self.s1[s, self.z] + self.yr[s, self.z].astype(f32)

        @pl.when(q + self.ny < self.total)
        def _():
            self.signal(self.cy, device(self.r, 1 - self.y, self.z, self.c))

        for o in (1, 2, 3):

            @pl.when(q >= self.nz)
            def _():
                pl.semaphore_wait(self.cz.at[o - 1], 1)

            self.copy_z(q, o).start()

    def stage3(self, q):
        s = lax.rem(q, self.nz)

        @pl.when(q >= self.nz)
        def _():
            self.copy_out(q - self.nz).wait()

        for o in (1, 2, 3):
            self.copy_z(q, o).wait()
        total = self.acc[s] + self.zr[s, 0].astype(f32) + self.zr[s, 1].astype(f32) + self.zr[s, 2].astype(f32)
        total = total.astype(bf16)
        self.go[s] = total
        total = total.astype(f32)
        self.sums[...] += jnp.sum((total * total).reshape(-1, 8, total.shape[-1]), 0).reshape(8, -1, 128).sum(1)

        @pl.when(q + self.nz < self.total)
        def _():
            for o in (1, 2, 3):
                self.signal(self.cz.at[3 - o], device(self.r, self.y, lax.rem(self.z + o, 4), self.c))

        self.copy_out(q).start()

    def tick(self, t, first, count):
        for lag, stage in reversed(list(zip(self.LAGS, (self.stage0, self.stage1, self.stage2, self.stage3), strict=True))):
            q = t - lag

            @pl.when((q >= 0) & (q < count))
            def _():
                stage(first + q)

    def finish(self):
        for i in range(self.nz):
            self.copy_out(self.total - self.nz + i).wait()


class Staged:
    def __init__(self, at):
        self.at = at

    def start(self, q):
        pass

    def wait(self, q):
        pass

    def read(self, q, b):
        return self.at(q, b)[...]


class Fetched:
    def __init__(self, source, buf, sems, slots):
        self.source, self.buf, self.sems, self.slots = source, buf, sems, slots

    def copies(self, q):
        s = lax.rem(q, self.slots)
        return [pltpu.make_async_copy(src, self.buf.at[s, b], self.sems.at[s, b]) for src, b in self.source(q)]

    def start(self, q):
        for copy in self.copies(q):
            copy.start()

    def wait(self, q):
        for copy in self.copies(q):
            copy.wait()

    def read(self, q, b):
        return self.buf[lax.rem(q, self.slots), b]


B = 640
NB = FF // B
DC, DP = 256, 4
HALF = 512
EC = 256
GS, DS = (2, 3, 3), (2, 2, 2)
ES = 3
STEPS = T // EC


def backward_kernel(
    dy_ref, h1_ref, a1_ref, a0_ref, gate1, up1, gate0, up0, mid1, mid0, wg_ref, wu_ref, wd_ref,
    g_out, d_out, sums_out, dd_ref,
    sums, dh, a, da, ga, ua, dmid, dgu, wgu, wdj, dwst, ddst, xo,
    s_dh, s_a, s_gu, s_mid, s_wgu, s_wd, s_dd, s_xo, *bufs,
):
    half = len(bufs) // 2
    r, y, z, c = place()
    cp = pltpu.make_async_copy

    load_dh = cp(dy_ref, dh, s_dh)
    load_dh.start()
    load_a1 = cp(a1_ref, a, s_a)
    load_a1.start()
    greet(r, y, z, c)
    sums[...] = jnp.zeros_like(sums)
    da[...] = jnp.zeros_like(da)

    def g_part(q):
        n = q // 2
        return lax.rem(n, 2), pl.ds(pl.multiple_of(lax.rem(q, 2) * B, 128), B)

    def g_source(q, c):
        s, cols = g_part(q)
        return [(dwst.at[s, :, c, :, cols], None)]

    def g_own(q, b):
        s, cols = g_part(q)
        return dwst.at[s, b, c, :, cols]

    def g_to(q):
        n = q // 2
        return g_out.at[n // NB * 2 + lax.rem(q, 2), :, pl.ds(pl.multiple_of(lax.rem(n, NB) * B, 128), B)]

    def d_source(q, c):
        m, p = q // DP, lax.rem(q, DP)
        cols = pl.ds(pl.multiple_of(p * DC, 128), DC)
        return [(dd_ref.at[m, pl.ds((2 * b + c) * 25, 25), :, cols], b) for b in range(8)]

    def d_to(q):
        m, p = q // DP, lax.rem(q, DP)
        return d_out.at[m, :, :, pl.ds(pl.multiple_of(p * DC, 128), DC)]

    gr = Reducer(g_source, Staged(g_own), g_to, sums, GS, 4 * NB, bufs[:half])
    dr = Reducer(d_source, Fetched(lambda q: d_source(q, c), xo, s_xo, DS[0]), d_to, sums, DS, 2 * DP, bufs[half:])

    for n, (gate, up, mid) in enumerate(((gate1, up1, mid1), (gate0, up0, mid0))):
        layer = 1 - n

        def load_mid(st):
            s = lax.rem(st, 2)
            return cp(mid.at[:, pl.ds(pl.multiple_of(lax.rem(st, NB) * B, 128), B)],
                      dgu.at[:, pl.ds(pl.multiple_of(s * B, 128), B)], s_mid.at[s])

        def write_dd(st):
            return cp(ddst.at[lax.rem(st, 2)],
                      dd_ref.at[n, pl.ds(lax.rem(st, NB) * (B // 8), B // 8), :, pl.ds(pl.multiple_of(st // NB * HALF, 128), HALF)],
                      s_dd.at[lax.rem(st, 2)])

        def load_wd(j):
            s = lax.rem(j, 2)
            return cp(wd_ref.at[layer, pl.ds(pl.multiple_of(j * B, 8), B)], wdj.at[s], s_wd.at[s])

        def load_wgu(j):
            cols = pl.ds(pl.multiple_of(j * B, 128), B)
            return cp(wg_ref.at[layer, :, cols], wgu.at[:, pl.ds(0, B)], s_wgu.at[0]), cp(wu_ref.at[layer, :, cols], wgu.at[:, pl.ds(B, B)], s_wgu.at[1])

        def load_gu(k):
            s, j, i = lax.rem(k, ES), k // STEPS, lax.rem(k, STEPS)
            at = (pl.ds(pl.multiple_of(i * EC, 8), EC), pl.ds(pl.multiple_of(j * B, 128), B))
            return cp(gate.at[at], ga.at[s], s_gu.at[s, 0]), cp(up.at[at], ua.at[s], s_gu.at[s, 1])

        load_mid(0).start()
        load_wd(0).start()
        for k in range(ES - 1):
            for copy in load_gu(k):
                copy.start()
        if n == 0:
            load_dh.wait()

        def down(st, _):
            @pl.when(st + 1 < 2 * NB)
            def _():
                load_mid(st + 1).start()

            load_mid(st).wait()
            s = lax.rem(st, 2)
            tile = dot(dgu[:, pl.ds(pl.multiple_of(s * B, 128), B)], dh[:, pl.ds(pl.multiple_of(st // NB * HALF, 128), HALF)], 0, 0)
            ddst[s] = tile.astype(bf16).reshape(B // 8, 8, HALF)

            @pl.when((st != 0) & (st != NB))
            def _():
                write_dd(st - 1).wait()

            write_dd(st).start()

            @pl.when((st == NB - 1) | (st == 2 * NB - 1))
            def _():
                write_dd(st).wait()

            @pl.when((st == 4) | (st == 6) | (st == 9))
            def _():
                dr.tick((st - 4) // 2, n * DP, DP)

            if n == 1:

                @pl.when(lax.rem(st, 2) == 0)
                def _():
                    gr.tick(10 + st // 2, 0, 2 * NB)

            return 0

        lax.fori_loop(0, 2 * NB, down, 0)

        if n == 0:
            load_a1.wait()
        else:
            cp(a0_ref, a, s_a).wait()

        def block(j, _):
            @pl.when(j + 1 < NB)
            def _():
                load_wd(j + 1).start()

            if n == 0:
                for copy in load_wgu(j):
                    copy.start()
            load_wd(j).wait()

            def dmids(i, _):
                rows = pl.ds(pl.multiple_of(i * 512, 8), 512)
                dmid[rows, :] = dot(dh[rows, :], wdj[lax.rem(j, 2)], 1, 1).astype(bf16)
                return 0

            lax.fori_loop(0, T // 512, dmids, 0)

            def act(i, _):
                k = j * STEPS + i

                @pl.when(k + ES - 1 < NB * STEPS)
                def _():
                    for copy in load_gu(k + ES - 1):
                        copy.start()

                for copy in load_gu(k):
                    copy.wait()
                s = lax.rem(k, ES)
                rows = pl.ds(pl.multiple_of(i * EC, 8), EC)
                dm = dmid[rows, :].astype(f32)
                ge = ga[s]
                sig = 0.5 + 0.5 * jnp.tanh(0.5 * ge)
                silu = ge * sig
                dgu[rows, 0:B] = (dm * ua[s] * (sig + silu * (1.0 - sig))).astype(bf16)
                dgu[rows, B : 2 * B] = (dm * silu).astype(bf16)
                return 0

            lax.fori_loop(0, STEPS, act, 0)

            dr.tick(3 + 2 * j, n * DP, DP)

            @pl.when(j >= 1)
            def _():
                gr.tick(2 * j - 1, n * 2 * NB, 2 * NB)

            def terms(i, _):
                rows = pl.ds(pl.multiple_of(i * 512, 128), 512)
                dwst[lax.rem(n * NB + j, 2), pl.ds(i * 4, 4)] = dot(a[:, rows], dgu[...], 0, 0).astype(bf16).reshape(4, 2, 64, 2 * B)
                return 0

            lax.fori_loop(0, D // 512, terms, 0)

            dr.tick(4 + 2 * j, n * DP, DP)
            gr.tick(2 * j, n * 2 * NB, 2 * NB)

            if n == 0:
                for copy in load_wgu(j):
                    copy.wait()

                def back(i, _):
                    rows = pl.ds(pl.multiple_of(i * 512, 8), 512)
                    da[rows, :] += dot(dgu[rows, :], wgu[...], 1, 1)
                    return 0

                lax.fori_loop(0, T // 512, back, 0)
            return 0

        lax.fori_loop(0, NB, block, 0)
        gr.tick(9, n * 2 * NB, 2 * NB)
        if n == 0:
            load_h = cp(h1_ref, a, s_a)
            load_h.start()
            load_h.wait()

            def norm(i, _):
                rows = pl.ds(pl.multiple_of(i * 128, 8), 128)
                wide = a[rows, :].astype(f32)
                d = da[rows, :].astype(bf16).astype(f32)
                scale = lax.rsqrt(jnp.mean(wide * wide, -1, keepdims=True) + 1e-6)
                inner = jnp.mean(d * wide, -1, keepdims=True)
                dn = (scale * d - wide * (scale * scale * scale * inner)).astype(bf16)
                dh[rows, :] = (dh[rows, :].astype(f32) + dn.astype(f32)).astype(bf16)
                return 0

            lax.fori_loop(0, T // 128, norm, 0)
            load_a0 = cp(a0_ref, a, s_a)
            load_a0.start()

    lax.fori_loop(10, 15, lambda t, _: (gr.tick(t, 2 * NB, 2 * NB), 0)[1], 0)
    dr.finish()
    gr.finish()
    sums_out[...] = sums[...]


def backward(dy, h1, a1, a0, gate1, up1, gate0, up0, mid1, mid0, wg, wu, wd):
    V, dma = pltpu.VMEM, pltpu.SemaphoreType.DMA
    return pl.pallas_call(
        backward_kernel,
        out_shape=(
            jax.ShapeDtypeStruct((4, 64, FF), bf16),
            jax.ShapeDtypeStruct((2, 25, 8, D), bf16),
            jax.ShapeDtypeStruct((8, 128), f32),
            jax.ShapeDtypeStruct((2, FF // 8, 8, D), bf16),
        ),
        in_specs=[pl.BlockSpec(memory_space=HBM)] * 13,
        out_specs=(pl.BlockSpec(memory_space=HBM), pl.BlockSpec(memory_space=HBM), pl.BlockSpec(memory_space=V), pl.BlockSpec(memory_space=HBM)),
        scratch_shapes=[
            V((8, 128), f32), V((T, D), bf16), V((T, D), bf16), V((T, D), f32), V((ES, EC, B), f32), V((ES, EC, B), f32),
            V((T, B), bf16), V((T, 2 * B), bf16), V((D, 2 * B), bf16), V((2, B, D), bf16), V((2, 8, 2, 64, 2 * B), bf16),
            V((2, B // 8, 8, HALF), bf16), V((DS[0], 8, 25, 8, DC), bf16),
            dma, dma, dma((ES, 2)), dma((2,)), dma((2,)), dma((2,)), dma((2,)), dma((DS[0], 8)),
        ] + Reducer.scratch((64, B), 1, GS) + Reducer.scratch((25, 8, DC), 8, DS),
        compiler_params=pltpu.CompilerParams(collective_id=0, has_side_effects=True, vmem_limit_bytes=67043328),
    )(dy, h1, a1, a0, gate1, up1, gate0, up0, mid1, mid0, wg, wu, wd)


def gather_kernel(sg, su, sd, og, ou, od, zs, zr, ys, yr, ds, dr, ls):
    r, y, z, c = place()
    greet(r, y, z, c)
    chunks = [(s, o, layer) for layer in range(2) for s, o in ((sg, og), (su, ou), (sd, od))]
    n = len(chunks)

    def block(y, z, c):
        return y * 8 + z * 2 + c

    def zat(o):
        return lax.rem(z + o, 4)

    partner, across = device(r, y, z, 1 - c), device(r, 1 - y, z, c)
    mine = block(y, z, c)
    sent = []

    def send(src, k, b, ssem, rsem, dev):
        _, o, layer = chunks[k]
        copy = pltpu.make_async_remote_copy(src, o.at[layer, b], ssem, rsem, device_id=dev, device_id_type=MESH)
        copy.start()
        sent.append(copy)

    def arrived(k, b, ssem, rsem, dev):
        _, o, layer = chunks[k]
        ref = o.at[layer, b]
        pltpu.make_async_remote_copy(ref, ref, ssem, rsem, device_id=dev, device_id_type=MESH).wait_recv()
        return ref

    local = []
    for k, (s, o, layer) in enumerate(chunks):
        for d in (1, 2, 3):
            send(s.at[layer], k, mine, zs.at[k, d - 1], zr.at[k, 3 - d], device(r, y, zat(d), c))
        send(s.at[layer], k, mine, ys.at[k, 0], yr.at[k, 0], across)
        send(s.at[layer], k, mine, ds.at[k, 0], dr.at[k, 0], partner)
        copy = pltpu.make_async_copy(s.at[layer], o.at[layer, mine], ls.at[k])
        copy.start()
        local.append(copy)
    for k in range(n + 1):
        if k < n:
            for d in (1, 2, 3):
                b = block(y, zat(d), c)
                ref = arrived(k, b, zs.at[k, d - 1], zr.at[k, d - 1], across)
                send(ref, k, b, ys.at[k, d], yr.at[k, d], across)
                send(ref, k, b, ds.at[k, d], dr.at[k, d], partner)
        if k >= 1:
            for d in range(4):
                b = block(1 - y, zat(d), c)
                ref = arrived(k - 1, b, ys.at[k - 1, d], yr.at[k - 1, d], across)
                send(ref, k - 1, b, ds.at[k - 1, 4 + d], dr.at[k - 1, 4 + d], partner)
    for k in range(n):
        for e in range(8):
            b = block(y if e < 4 else 1 - y, zat(e % 4), 1 - c)
            arrived(k, b, ds.at[k, e], dr.at[k, e], partner)
    for copy in sent:
        copy.wait_send()
    for copy in local:
        copy.wait()


def all_gather(sg, su, sd):
    dma = pltpu.SemaphoreType.DMA
    out = pl.pallas_call(
        gather_kernel,
        out_shape=(
            jax.ShapeDtypeStruct((2, 16, 64, FF), bf16),
            jax.ShapeDtypeStruct((2, 16, 64, FF), bf16),
            jax.ShapeDtypeStruct((2, 16, 200, D), bf16),
        ),
        in_specs=[pl.BlockSpec(memory_space=pltpu.VMEM)] * 3,
        out_specs=[pl.BlockSpec(memory_space=HBM)] * 3,
        scratch_shapes=[dma((6, 3)), dma((6, 3)), dma((6, 4)), dma((6, 4)), dma((6, 8)), dma((6, 8)), dma((6,))],
        compiler_params=pltpu.CompilerParams(collective_id=1, has_side_effects=True),
    )(sg, su, sd)
    return out[0].reshape(2, D, FF), out[1].reshape(2, D, FF), out[2].reshape(2, FF, D)


def normed(h):
    wide = h.astype(f32)
    return (wide * lax.rsqrt(jnp.mean(wide**2, -1, keepdims=True) + 1e-6)).astype(bf16)


def forward(x, wg, wu, wd):
    h, kept = x, []
    for i in range(2):
        a = normed(h)
        gate, up = dot(a, wg[i], 1, 0), dot(a, wu[i], 1, 0)
        mid = (jax.nn.silu(gate) * up).astype(bf16)
        kept.append((a, gate, up, mid))
        if i == 0:
            h = h + dot(mid, wd[i], 1, 0).astype(bf16)
    return h, *kept


def adamw(w, m, v, g):
    m = 0.9 * m + 0.1 * g
    v = 0.95 * v + 0.05 * g * g
    step = m * lax.rsqrt(v + 1e-8) + 0.1 * w
    return (w - 0.02 * step).astype(bf16), m, v


def solution(mesh):
    def step(x, dy, wg, wu, wd, mg, mu, md, vg, vu, vd):
        h1, (a0, gate0, up0, mid0), (a1, gate1, up1, mid1) = forward(x[0], wg, wu, wd)
        gg, gd, sums, _ = backward(dy[0], h1, a1, a0, gate1, up1, gate0, up0, mid1, mid0, wg, wu, wd)
        gd = gd.reshape(2, 200, D)
        squares = lax.psum(jnp.sum(sums), "dp")
        factor = jnp.minimum(1.0, 0.5 * lax.rsqrt(squares / (6 * D * FF) + 1e-30))
        me = lax.axis_index("dp")
        new = []
        for w, m, v, g in ((wg, mg, vg, gg[2::-2]), (wu, mu, vu, gg[3::-2]), (wd, md, vd, gd[::-1])):
            rows = m.shape[1]
            mine = lax.dynamic_slice_in_dim(w, me * rows, rows, 1)
            new.append(adamw(mine.astype(f32), m, v, g.astype(f32) * factor))
        weights = all_gather(*(n[0] for n in new))
        return (*weights, *(n[1] for n in new), *(n[2] for n in new))

    seq, rep, own = P(("rep", "dp")), P("rep"), P("rep", "dp")
    return jax.shard_map(
        step,
        mesh=mesh,
        in_specs=(seq, seq, P(), P(), P(), *[P(None, "dp")] * 6),
        out_specs=(rep,) * 3 + (own,) * 6,
        check_vma=False,
    )
```

```python
import functools

import jax
import jax.numpy as jnp
from jax import lax
from jax.experimental import pallas as pl
from jax.experimental.pallas import tpu as pltpu
from jax.sharding import PartitionSpec as P

MESH = pl.DeviceIdType.MESH
HBM, VMEM = pltpu.HBM, pltpu.VMEM
DMA, REGULAR = pltpu.SemaphoreType.DMA, pltpu.SemaphoreType.REGULAR
bf16, f32 = jnp.bfloat16, jnp.float32
D, FF, T = 1024, 3200, 2048
B = 640
NB = FF // B
R = 512
ring = lax.rem


def place():
    me = lax.axis_index("dp")
    return lax.axis_index("rep"), me // 8, ring(me // 2, 4), ring(me, 2)


def device(r, y, z, c):
    return (r, y * 8 + z * 2 + c)


def greet(r, y, z, c):
    bar = pltpu.get_barrier_semaphore()
    peers = [device(r, y, z, 1 - c), device(r, 1 - y, z, c)] + [device(r, y, ring(z + o, 4), c) for o in (1, 2, 3)]
    for p in peers:
        signal(bar, p)
    pl.semaphore_wait(bar, len(peers))


def signal(sem, dev):
    pl.semaphore_signal(sem, 1, device_id=dev, device_id_type=MESH)


def remote(src, dst, ssem, rsem, dev):
    return pltpu.make_async_remote_copy(src, dst, ssem, rsem, device_id=dev, device_id_type=MESH)


def start(copies):
    for copy in copies:
        copy.start()


def finish(copies):
    for copy in copies:
        copy.wait()


def loop(n, body):
    lax.fori_loop(0, n, lambda i, carry: (body(i), carry)[1], None)


def when(ok):
    return pl.when(ok)


def part(i, n):
    return pl.ds(pl.multiple_of(i * n, n), n)


def dot(a, b, ca, cb):
    return lax.dot_general(a, b, (((ca,), (cb,)), ((), ())), preferred_element_type=f32)


nn = functools.partial(dot, ca=1, cb=0)
nt = functools.partial(dot, ca=1, cb=1)
tn = functools.partial(dot, ca=0, cb=0)


def normed(h):
    wide = h.astype(f32)
    return (wide * lax.rsqrt(jnp.mean(wide * wide, -1, keepdims=True) + 1e-6)).astype(bf16)


N = 128
CHUNKS = T // R
STEPS = NB * CHUNKS
FS = 4


def forward_kernel(
    x_ref, wg_ref, wu_ref, wd_ref,
    a0_ref, a1_ref, h1_ref, p0, s0, m0, p1, s1, m1,
    x, a, total, wgu, wdj, g, stp, sts, sta, stb, s_x, s_out, s_wg, s_wu, s_wd, s_p, s_s, s_m,
):
    cp = pltpu.make_async_copy

    def load_w(n):
        s, cols = ring(n, 2), part(ring(n, NB), B)
        return (cp(wg_ref.at[n // NB, :, cols], wgu.at[s, :, pl.ds(0, B)], s_wg.at[s]),
                cp(wu_ref.at[n // NB, :, cols], wgu.at[s, :, pl.ds(B, B)], s_wu.at[s]))

    def load_wd(j):
        s = ring(j, 2)
        return cp(wd_ref.at[0, part(j, B)], wdj.at[s], s_wd.at[s])

    load_x = cp(x_ref, x, s_x)
    load_x.start()
    start(load_w(0))
    total[...] = jnp.zeros_like(total)
    stb[...] = jnp.zeros_like(stb)
    load_wd(0).start()
    load_x.wait()

    def norm(i):
        rows = part(i, N)
        a[rows, :] = normed(x[rows, :])

    loop(T // N, norm)
    out_a0 = cp(a, a0_ref, s_out.at[0])
    out_a0.start()
    load_wd(0).wait()
    for layer, (p, s, m) in enumerate(((p0, s0, m0), (p1, s1, m1))):

        def writes(k, even):
            t, u, at = ring(k, FS), ring(k // 2, FS // 2), (part(ring(k, CHUNKS), R), part(k // CHUNKS, B))
            return cp(stp.at[t], p.at[at], s_p.at[t]), cp(sts.at[t], s.at[at], s_s.at[t]), cp((sta if even else stb).at[u], m.at[at], s_m.at[t])

        def down(k, even):
            mid = (sta if even else stb)[ring(k // 2, FS // 2)]
            total[part(ring(k, CHUNKS), R), :] += nn(mid, wdj[ring(k // CHUNKS, 2)])

        def step(k, even):
            j, i, t = k // CHUNKS, ring(k, CHUNKS), ring(k, FS)
            n = layer * NB + j

            @when(i == 0)
            def _():
                finish(load_w(n))

                @when(n + 1 < 2 * NB)
                def _():
                    start(load_w(n + 1))

            if layer == 0:

                @when(i == 1)
                def _():
                    @when(j > 0)
                    def _():
                        load_wd(j).wait()

                    @when(j + 1 < NB)
                    def _():
                        load_wd(j + 1).start()

            @when(k >= FS)
            def _():
                finish(writes(k - FS, even))

            g[...] = nn(a[part(i, R), :], wgu[ring(n, 2)])
            if layer == 0:
                down(jnp.where(k == 0, STEPS - 1, k - 1), not even)
            gate, up = g[:, :B], g[:, B:]
            sig = 0.5 + 0.5 * jnp.tanh(0.5 * gate)
            silu = gate * sig
            (sta if even else stb)[ring(k // 2, FS // 2)] = (silu * up).astype(bf16)
            stp[t] = up * (sig + silu * (1.0 - sig))
            sts[t] = silu
            start(writes(k, even))

        def steps(i):
            step(2 * i, True)
            step(2 * i + 1, False)

        loop(STEPS // 2, steps)
        if layer == 0:
            down(STEPS - 1, False)
        for k in range(STEPS - FS, STEPS):
            finish(writes(k, k % 2 == 0))
        if layer == 0:
            out_a0.wait()
            def joint(i):
                rows = part(i, N)
                h = (x[rows, :].astype(f32) + total[rows, :].astype(bf16).astype(f32)).astype(bf16)
                x[rows, :] = h
                a[rows, :] = normed(h)

            loop(T // N, joint)
            outs = cp(x, h1_ref, s_out.at[0]), cp(a, a1_ref, s_out.at[1])
            start(outs)
    finish(outs)


def forward(x, wg, wu, wd):
    states, wide, mid = (jax.ShapeDtypeStruct((T, n), t) for n, t in ((D, bf16), (FF, f32), (FF, bf16)))
    two = (2,)
    return pl.pallas_call(
        forward_kernel,
        out_shape=(states,) * 3 + (wide, wide, mid) * 2,
        in_specs=[pl.BlockSpec(memory_space=HBM)] * 4,
        out_specs=(pl.BlockSpec(memory_space=HBM),) * 9,
        scratch_shapes=[
            VMEM((T, D), bf16), VMEM((T, D), bf16), VMEM((T, D), f32), VMEM((2, D, 2 * B), bf16), VMEM((2, B, D), bf16),
            VMEM((R, 2 * B), f32), VMEM((FS, R, B), f32), VMEM((FS, R, B), f32), VMEM((FS // 2, R, B), bf16), VMEM((FS // 2, R, B), bf16),
            DMA, DMA(two), DMA(two), DMA(two), DMA(two), DMA((FS,)), DMA((FS,)), DMA((FS,)),
        ],
        compiler_params=pltpu.CompilerParams(vmem_limit_bytes=67043328),
    )(x, wg, wu, wd)


class Reducer:
    LAGS = (0, 1, 3, 5)

    def __init__(self, source, own, out, sums, slots, total, bufs):
        self.source, self.own, self.out, self.sums, self.total = source, own, out, sums, total
        self.nx, self.ny, self.nz = slots
        (self.xr, self.ys, self.yr, self.s1, self.acc, self.zs, self.zr, self.go,
         self.xss, self.xrs, self.yss, self.yrs, self.zss, self.zrs, self.gos, self.cx, self.cy, self.cz) = bufs
        r, y, self.z, c = place()
        self.y, self.c = y, c
        self.partner, self.across = device(r, y, self.z, 1 - c), device(r, 1 - y, self.z, c)
        self.along = [device(r, y, self.zat(o), c) for o in (1, 2, 3)]

    def zat(self, o):
        return ring(self.z + o, 4)

    @staticmethod
    def scratch(shape, parts, slots):
        nx, ny, nz = slots
        return [
            VMEM((nx, 8, *shape), bf16), VMEM((ny, 4, *shape), bf16), VMEM((ny, 4, *shape), bf16), VMEM((ny, 4, *shape), f32),
            VMEM((nz, *shape), f32), VMEM((nz, 3, *shape), bf16), VMEM((nz, 3, *shape), bf16), VMEM((nz, *shape), bf16),
            DMA((nx, parts)), DMA((nx, parts)), DMA((ny,)), DMA((ny,)), DMA((nz, 3)), DMA((nz, 3)), DMA((nz,)), REGULAR, REGULAR, REGULAR((3,)),
        ]

    def copies_x(self, q):
        s = ring(q, self.nx)
        return [
            remote(src, self.xr.at[s] if b is None else self.xr.at[s, b], self.xss.at[s, b or 0], self.xrs.at[s, b or 0], self.partner)
            for src, b in self.source(q, 1 - self.c)
        ]

    def copy_y(self, q):
        s = ring(q, self.ny)
        return remote(self.ys.at[s], self.yr.at[s], self.yss.at[s], self.yrs.at[s], self.across)

    def copies_z(self, q):
        s = ring(q, self.nz)
        return [remote(self.zs.at[s, i], self.zr.at[s, 2 - i], self.zss.at[s, i], self.zrs.at[s, 2 - i], dev) for i, dev in enumerate(self.along)]

    def copy_out(self, q):
        s = ring(q, self.nz)
        return pltpu.make_async_copy(self.go.at[s], self.out(q), self.gos.at[s])

    def stage0(self, q):
        @when(q >= self.nx)
        def _():
            pl.semaphore_wait(self.cx, 1)

        start(self.copies_x(q))
        self.own.start(q)

    def stage1(self, q):
        x, s = ring(q, self.nx), ring(q, self.ny)
        self.own.wait(q)
        finish(self.copies_x(q))

        def add(i):
            b = (1 - self.y) * 4 + i
            self.ys[s, i] = (self.own.read(q, b).astype(f32) + self.xr[x, b].astype(f32)).astype(bf16)
            b = self.y * 4 + i
            self.s1[s, i] = self.own.read(q, b).astype(f32) + self.xr[x, b].astype(f32)

        loop(4, add)

        @when(q + self.nx < self.total)
        def _():
            signal(self.cx, self.partner)

        @when(q >= self.ny)
        def _():
            pl.semaphore_wait(self.cy, 1)

        self.copy_y(q).start()

    def stage2(self, q):
        s, t = ring(q, self.ny), ring(q, self.nz)
        self.copy_y(q).wait()
        for i in range(3):
            b = self.zat(i + 1)
            self.zs[t, i] = (self.s1[s, b] + self.yr[s, b].astype(f32)).astype(bf16)
        self.acc[t] = self.s1[s, self.z] + self.yr[s, self.z].astype(f32)

        @when(q + self.ny < self.total)
        def _():
            signal(self.cy, self.across)

        @when(q >= self.nz)
        def _():
            for i in range(3):
                pl.semaphore_wait(self.cz.at[i], 1)

        start(self.copies_z(q))

    def stage3(self, q):
        s = ring(q, self.nz)

        @when(q >= self.nz)
        def _():
            self.copy_out(q - self.nz).wait()

        finish(self.copies_z(q))
        total = self.acc[s]
        for i in range(3):
            total += self.zr[s, i].astype(f32)
        total = total.astype(bf16)
        self.go[s] = total
        total = total.astype(f32)
        self.sums[...] += jnp.sum((total * total).reshape(-1, 8, total.shape[-1]), 0).reshape(8, -1, 128).sum(1)

        @when(q + self.nz < self.total)
        def _():
            for i, dev in enumerate(self.along):
                signal(self.cz.at[2 - i], dev)

        self.copy_out(q).start()

    def tick(self, t, first, count):
        for lag, stage in zip(self.LAGS[::-1], (self.stage3, self.stage2, self.stage1, self.stage0), strict=True):
            q = t - lag
            when((q >= 0) & (q < count))(functools.partial(stage, first + q))

    def close(self):
        finish([self.copy_out(self.total - self.nz + i) for i in range(self.nz)])


class Staged:
    def __init__(self, at):
        self.at = at

    def start(self, q):
        pass

    wait = start

    def read(self, q, b):
        return self.at(q, b)[...]


class Fetched:
    def __init__(self, source, buf, sems, slots):
        self.source, self.buf, self.sems, self.slots = source, buf, sems, slots

    def copies(self, q):
        s = ring(q, self.slots)
        return [pltpu.make_async_copy(src, self.buf.at[s, b], self.sems.at[s, b]) for src, b in self.source(q)]

    def start(self, q):
        start(self.copies(q))

    def wait(self, q):
        finish(self.copies(q))

    def read(self, q, b):
        return self.buf[ring(q, self.slots), b]


DC, DP = 256, 4
GP = 2 * NB
HALF = 512
GS, DS = (2, 3, 3), (2, 2, 2)
EC, ES = 256, 6
E = T // EC
ROWS = B // 8


def backward_kernel(
    dy_ref, h1_ref, a1_ref, a0_ref, p1, s1, mid1, p0, s0, mid0, wg_ref, wu_ref, wd_ref,
    g_out, d_out, sums_out, dd_ref,
    sums, dh, a, da, pa, sa, dgu, wgu, wdj, dwst, ddst, xo,
    tot, got, s_tot, s_tot_in, s_dh, s_a, s_ps, s_mid, s_wgu, s_wd, s_dd, s_xo, *bufs,
):
    half = len(bufs) // 2
    r, y, z, c = place()
    cp = pltpu.make_async_copy

    load_dh = cp(dy_ref, dh, s_dh)
    load_a = cp(a1_ref, a, s_a)
    load_h, load_a0 = cp(h1_ref, a, s_a), cp(a0_ref, a, s_a)
    load_dh.start()
    load_a.start()
    greet(r, y, z, c)
    sums[...] = jnp.zeros_like(sums)
    da[...] = jnp.zeros_like(da)

    def g_part(q):
        return ring(q // 2, 2), part(ring(q, 2), B)

    def g_source(q, c):
        s, cols = g_part(q)
        return [(dwst.at[s, :, c, :, cols], None)]

    def g_own(q, b):
        s, cols = g_part(q)
        return dwst.at[s, b, c, :, cols]

    def g_to(q):
        n = q // 2
        return g_out.at[ring(q, 2), 1 - n // NB, :, part(ring(n, NB), B)]

    def d_source(q, c):
        return [(dd_ref.at[q // DP, pl.ds((2 * b + c) * 25, 25), :, part(ring(q, DP), DC)], b) for b in range(8)]

    def d_to(q):
        return d_out.at[1 - q // DP, :, :, part(ring(q, DP), DC)]

    gr = Reducer(g_source, Staged(g_own), g_to, sums, GS, 2 * GP, bufs[:half])
    dr = Reducer(d_source, Fetched(lambda q: d_source(q, c), xo, s_xo, DS[0]), d_to, sums, DS, 2 * DP, bufs[half:])

    for n, (p, s, mid) in enumerate(((p1, s1, mid1), (p0, s0, mid0))):
        layer, d_first, g_first = 1 - n, n * DP, n * GP

        def load_mid(st):
            t = ring(st, 2)
            return cp(mid.at[:, part(ring(st, NB), B)], dgu.at[:, part(t, B)], s_mid.at[t])

        def write_dd(i, h, t):
            return cp(ddst.at[t], dd_ref.at[n, part(i, ROWS), :, part(h, HALF)], s_dd.at[t])

        def load_wd(j):
            return cp(wd_ref.at[layer, part(j, B)], wdj, s_wd)

        def load_wgu(j):
            return [cp(w.at[layer, :, part(j, B)], wgu.at[:, part(i, B)], s_wgu.at[i]) for i, w in enumerate((wg_ref, wu_ref))]

        def load_ps(k):
            t, at = ring(k, ES), (part(ring(k, E), EC), part(k // E, B))
            return cp(p.at[at], pa.at[t], s_ps.at[t, 0]), cp(s.at[at], sa.at[t], s_ps.at[t, 1])

        load_mid(0).start()
        load_wd(0).start()
        for k in range(ES - 1):
            start(load_ps(k))
        if n == 0:
            load_dh.wait()

        def tile(t, st, h):
            ddst[t] = tn(dgu[:, part(ring(st, 2), B)], dh[:, part(h, HALF)]).astype(bf16).reshape(ROWS, 8, HALF)

        def load_next(st, last):
            @when(st < last)
            def _():
                load_mid(st + 1).start()

            load_mid(st).wait()

        def down_by_half(st):
            load_next(st, 2 * NB - 1)
            t, i, h = ring(st, 2), ring(st, NB), st // NB
            tile(t, st, h)

            @when((st != 0) & (st != NB))
            def _():
                write_dd(ring(st - 1, NB), h, 1 - t).wait()

            write_dd(i, h, t).start()

            @when(i == NB - 1)
            def _():
                write_dd(i, h, t).wait()

            @when((st == 4) | (st == 6) | (st == 9))
            def _():
                dr.tick((st - 4) // 2, d_first, DP)

        def down(i):
            load_next(i, NB - 1)

            def each(h):
                @when(i > 0)
                def _():
                    write_dd(i - 1, h, h).wait()

                tile(h, i, h)
                write_dd(i, h, h).start()

            loop(2, each)
            gr.tick(GP + i, 0, GP)

        if n == 0:
            loop(2 * NB, down_by_half)
            load_a.wait()
        else:
            loop(NB, down)
            finish([write_dd(NB - 1, h, h) for h in range(2)])
            dr.tick(0, d_first, DP)
            load_a0.wait()
        ahead = 1 if n else 3

        def block(j):
            if n == 0:
                start(load_wgu(j))
            load_wd(j).wait()

            def act(i):
                k = j * E + i

                @when(k + ES - 1 < NB * E)
                def _():
                    start(load_ps(k + ES - 1))

                finish(load_ps(k))
                t, rows = ring(k, ES), part(i, EC)
                dm = dgu[rows, :B].astype(f32)
                dgu[rows, :B] = (dm * pa[t]).astype(bf16)
                dgu[rows, B:] = (dm * sa[t]).astype(bf16)

            def dmids(i):
                rows = part(i, R)
                dgu[rows, :B] = nt(dh[rows, :], wdj[...]).astype(bf16)
                loop(R // EC, lambda e: act(i * (R // EC) + e))

            loop(CHUNKS, dmids)

            @when(j + 1 < NB)
            def _():
                load_wd(j + 1).start()

            dr.tick(ahead + 2 * j, d_first, DP)

            @when(j >= 1)
            def _():
                gr.tick(2 * j - 1, g_first, GP)

            def terms(i):
                dwst[ring(n * NB + j, 2), part(i, 4)] = tn(a[:, part(i, R)], dgu[...]).astype(bf16).reshape(4, 2, 64, 2 * B)

            loop(D // R, terms)

            dr.tick(ahead + 1 + 2 * j, d_first, DP)
            gr.tick(2 * j, g_first, GP)

            if n == 0:
                finish(load_wgu(j))

                def back(i):
                    rows = part(i, R)
                    da[rows, :] += nt(dgu[rows, :], wgu[...])

                loop(CHUNKS, back)

        loop(NB, block)
        gr.tick(GP - 1, g_first, GP)
        if n == 0:
            load_h.start()
            load_h.wait()

            def norm(i):
                rows = part(i, N)
                wide = a[rows, :].astype(f32)
                d = da[rows, :].astype(bf16).astype(f32)
                scale = lax.rsqrt(jnp.mean(wide * wide, -1, keepdims=True) + 1e-6)
                inner = jnp.mean(d * wide, -1, keepdims=True)
                dn = (scale * d - wide * (scale * scale * scale * inner)).astype(bf16)
                dh[rows, :] = (dh[rows, :].astype(f32) + dn.astype(f32)).astype(bf16)

            loop(T // N, norm)
            load_a0.start()

    loop(NB, lambda t: gr.tick(GP + t, GP, GP))
    dr.close()
    gr.close()

    tot[0] = sums[...]
    for i, dev in enumerate((gr.partner, gr.across)):
        copy = remote(tot.at[i], got.at[i], s_tot.at[i], s_tot_in.at[i], dev)
        copy.start()
        copy.wait()
        tot[i + 1] = tot[i] + got[i]
    copies = [remote(tot.at[2], got.at[2 + z], s_tot.at[2 + i], s_tot_in.at[4 - i], dev) for i, dev in enumerate(gr.along)]
    start(copies)
    finish(copies)
    got[2 + z] = tot[2]
    sums_out[...] = got[2] + got[3] + got[4] + got[5]


def backward(*arrays):
    return pl.pallas_call(
        backward_kernel,
        out_shape=(
            jax.ShapeDtypeStruct((2, 2, 64, FF), bf16),
            jax.ShapeDtypeStruct((2, 25, 8, D), bf16),
            jax.ShapeDtypeStruct((8, 128), f32),
            jax.ShapeDtypeStruct((2, FF // 8, 8, D), bf16),
        ),
        in_specs=[pl.BlockSpec(memory_space=HBM)] * len(arrays),
        out_specs=tuple(pl.BlockSpec(memory_space=m) for m in (HBM, HBM, VMEM, HBM)),
        scratch_shapes=[
            VMEM((8, 128), f32), VMEM((T, D), bf16), VMEM((T, D), bf16), VMEM((T, D), f32), VMEM((ES, EC, B), f32), VMEM((ES, EC, B), f32),
            VMEM((T, 2 * B), bf16), VMEM((D, 2 * B), bf16), VMEM((B, D), bf16), VMEM((2, 8, 2, 64, 2 * B), bf16),
            VMEM((2, ROWS, 8, HALF), bf16), VMEM((DS[0], 8, 25, 8, DC), bf16),
            VMEM((3, 8, 128), f32), VMEM((6, 8, 128), f32), DMA((5,)), DMA((5,)),
            DMA, DMA, DMA((ES, 2)), DMA((2,)), DMA((2,)), DMA, DMA((2,)), DMA((DS[0], 8)),
        ] + Reducer.scratch((64, B), 1, GS) + Reducer.scratch((25, 8, DC), 8, DS),
        compiler_params=pltpu.CompilerParams(collective_id=0, has_side_effects=True, vmem_limit_bytes=67043328),
    )(*arrays)


def gather_kernel(sg, su, sd, og, ou, od, zss, zrs, yss, yrs, dss, drs, ls):
    r, y, z, c = place()
    greet(r, y, z, c)
    chunks = [(s, o, layer) for layer in range(2) for s, o in ((sg, og), (su, ou), (sd, od))]
    last = len(chunks) - 1
    entries = [(k, y) for k in range(last + 1)] + [(last, 1 - y)]
    partner, across = device(r, y, z, 1 - c), device(r, 1 - y, z, c)
    beside = device(r, y, ring(z + 1, 4), c), device(r, y, ring(z + 3, 4), c)
    sides = range(2)
    goes_on = z < 3, z > 0

    def there(d, side):
        return z + d <= 3 if side else z >= d

    def at(d, side):
        return z + d if side else z - d

    def block(k, row, zz, c=c):
        return chunks[k][1].at[chunks[k][2], row * 8 + zz * 2 + c]

    def along(src, e, zz, d, side):
        k, row = entries[e]
        when(goes_on[side])(remote(src, block(k, row, zz), zss.at[e, d - 1, side], zrs.at[e, d - 1, side], beside[side]).start)

    def over(src, k, zz, w):
        remote(src, block(k, y, zz), yss.at[k, w], yrs.at[k, w], across).start()

    def pair(src, k, row, zz):
        remote(src, block(k, row, zz), dss.at[k, row * 4 + zz], drs.at[k, row * 4 + zz], partner).start()

    def arrived(ref, sem):
        remote(ref, ref, sem, sem, partner).wait_recv()
        return ref

    def left(ref, sem):
        remote(ref, ref, sem, sem, partner).wait_send()

    def which(d, side):
        return 2 * d - 1 + side

    own = [s.at[layer] for s, _, layer in chunks]
    for k in [last, *range(last)]:
        over(own[k], k, z, 0)
    kept = [pltpu.make_async_copy(src, block(k, y, z), ls.at[k]) for k, src in enumerate(own)]
    for k, src in enumerate(own):
        for side in sides:
            along(src, k, z, 1, side)
        pair(src, k, y, z)
        kept[k].start()
    src = arrived(block(last, 1 - y, z), yrs.at[last, 0])
    for side in sides:
        along(src, last + 1, z, 1, side)
    pair(src, last, 1 - y, z)

    def crossed(d, k):
        for side in sides[: 1 + min(d, 1)]:

            def hand(zz, w):
                pair(arrived(block(k, 1 - y, zz), yrs.at[k, w]), k, 1 - y, zz)

            if d:
                when(there(d, side))(functools.partial(hand, at(d, side), which(d, side)))
            else:
                hand(z, 0)

    for d in (1, 2, 3):
        for e, (k, row) in enumerate(entries):
            for side in sides:

                @when(there(d, side))
                def _():
                    zz = at(d, side)
                    src = arrived(block(k, row, zz), zrs.at[e, d - 1, side])
                    if d < 3:
                        along(src, e, zz, d + 1, side)
                    if k != last:
                        over(src, k, zz, which(d, side))
                    pair(src, k, row, zz)

            if k != last:
                crossed(d - 1, k)
    for k in range(last):
        crossed(3, k)

    for k in range(last + 1):
        for b in range(8):
            left(arrived(block(k, 0, b, 1 - c), drs.at[k, b]), dss.at[k, b])
        left(own[k], yss.at[k, 0])
    for d in range(3):
        for side in sides:
            for e in range(len(entries)):
                when(goes_on[side] & there(d, side))(functools.partial(left, own[entries[e][0]], zss.at[e, d, side]))
            for k in range(last):
                when(there(d + 1, side))(functools.partial(left, own[k], yss.at[k, which(d + 1, side)]))
    finish(kept)


def all_gather(*shards):
    out = pl.pallas_call(
        gather_kernel,
        out_shape=[jax.ShapeDtypeStruct((2, 16, *s.shape[1:]), bf16) for s in shards],
        in_specs=[pl.BlockSpec(memory_space=HBM)] * 3,
        out_specs=[pl.BlockSpec(memory_space=pl.ANY)] * 3,
        scratch_shapes=[DMA((7, 3, 2)), DMA((7, 3, 2)), DMA((6, 7)), DMA((6, 7)), DMA((6, 8)), DMA((6, 8)), DMA((6,))],
        compiler_params=pltpu.CompilerParams(collective_id=1, has_side_effects=True, vmem_limit_bytes=2**23),
    )(*shards)
    return [o.reshape(2, -1, o.shape[-1]) for o in out]


def adamw(w, m, v, g):
    m = 0.9 * m + 0.1 * g
    v = 0.95 * v + 0.05 * g * g
    step = m * lax.rsqrt(v + 1e-8) + 0.1 * w
    return (w - 0.02 * step).astype(bf16), m, v


def solution(mesh):
    def step(x, dy, wg, wu, wd, mg, mu, md, vg, vu, vd):
        a0, a1, h1, p0, s0, mid0, p1, s1, mid1 = forward(x[0], wg, wu, wd)
        gg, gd, sums, _ = backward(dy[0], h1, a1, a0, p1, s1, mid1, p0, s0, mid0, wg, wu, wd)
        factor = jnp.minimum(1.0, 0.5 * lax.rsqrt(jnp.sum(sums) / (6 * D * FF) + 1e-30))
        me = lax.axis_index("dp")
        new = []
        for w, m, v, g in ((wg, mg, vg, gg[0]), (wu, mu, vu, gg[1]), (wd, md, vd, gd.reshape(2, 200, D))):
            rows = m.shape[1]
            mine = lax.dynamic_slice_in_dim(w, me * rows, rows, 1)
            new.append(adamw(mine.astype(f32), m, v, g.astype(f32) * factor))
        weights = all_gather(*(n[0] for n in new))
        return (*weights, *(n[1] for n in new), *(n[2] for n in new))

    seq, rep, own = P(("rep", "dp")), P("rep"), P("rep", "dp")
    return jax.shard_map(
        step,
        mesh=mesh,
        in_specs=(seq, seq, P(), P(), P(), *[P(None, "dp")] * 6),
        out_specs=(rep,) * 3 + (own,) * 6,
        check_vma=False,
    )
```

```python
import functools

import jax
import jax.numpy as jnp
from jax import lax
from jax.experimental import pallas as pl
from jax.experimental.pallas import tpu as pltpu
from jax.sharding import PartitionSpec as P

MESH = pl.DeviceIdType.MESH
HBM, VMEM = pltpu.HBM, pltpu.VMEM
DMA, REGULAR = pltpu.SemaphoreType.DMA, pltpu.SemaphoreType.REGULAR
bf16, f32 = jnp.bfloat16, jnp.float32
D, FF, T = 1024, 3200, 2048
B = 640
NB = FF // B
R = 512
ring = lax.rem


def place():
    me = lax.axis_index("dp")
    return lax.axis_index("rep"), me // 8, ring(me // 2, 4), ring(me, 2)


def device(r, y, z, c):
    return (r, y * 8 + z * 2 + c)


def greet(r, y, z, c):
    bar = pltpu.get_barrier_semaphore()
    peers = [device(r, y, z, 1 - c), device(r, 1 - y, z, c)] + [device(r, y, ring(z + o, 4), c) for o in (1, 2, 3)]
    for p in peers:
        signal(bar, p)
    pl.semaphore_wait(bar, len(peers))


def signal(sem, dev):
    pl.semaphore_signal(sem, 1, device_id=dev, device_id_type=MESH)


def remote(src, dst, ssem, rsem, dev):
    return pltpu.make_async_remote_copy(src, dst, ssem, rsem, device_id=dev, device_id_type=MESH)


def start(copies):
    for copy in copies:
        copy.start()


def finish(copies):
    for copy in copies:
        copy.wait()


def loop(n, body):
    lax.fori_loop(0, n, lambda i, carry: (body(i), carry)[1], None)


def when(ok):
    return pl.when(ok)


def part(i, n):
    return pl.ds(pl.multiple_of(i * n, n), n)


def dot(a, b, ca, cb):
    return lax.dot_general(a, b, (((ca,), (cb,)), ((), ())), preferred_element_type=f32)


nn = functools.partial(dot, ca=1, cb=0)
nt = functools.partial(dot, ca=1, cb=1)
tn = functools.partial(dot, ca=0, cb=0)


def normed(h):
    wide = h.astype(f32)
    return (wide * lax.rsqrt(jnp.mean(wide * wide, -1, keepdims=True) + 1e-6)).astype(bf16)


N = 128
CHUNKS = T // R
STEPS = NB * CHUNKS
FS = 4


def forward_kernel(
    x_ref, wg_ref, wu_ref, wd_ref,
    a0_ref, a1_ref, h1_ref, p0, s0, m0, p1, s1, m1,
    x, a, mid, wgu, wd, g, stp, sts, s_x, s_out, s_wg, s_wu, s_wd, s_p, s_s, s_m,
):
    cp = pltpu.make_async_copy

    def load_w(n):
        s, cols = ring(n, 2), part(ring(n, NB), B)
        return (cp(wg_ref.at[n // NB, :, cols], wgu.at[s, :, pl.ds(0, B)], s_wg.at[s]),
                cp(wu_ref.at[n // NB, :, cols], wgu.at[s, :, pl.ds(B, B)], s_wu.at[s]))

    load_x, load_wd = cp(x_ref, x, s_x), cp(wd_ref.at[0], wd, s_wd)
    load_x.start()
    start(load_w(0))
    load_wd.start()
    load_x.wait()

    def norm(i):
        rows = part(i, N)
        a[rows, :] = normed(x[rows, :])

    loop(T // N, norm)
    out_a0 = cp(a, a0_ref, s_out.at[0])
    out_a0.start()
    for layer, (p, s, m) in enumerate(((p0, s0, m0), (p1, s1, m1))):

        def writes(k):
            t, at = ring(k, FS), (part(ring(k, CHUNKS), R), part(k // CHUNKS, B))
            return cp(stp.at[t], p.at[at], s_p.at[t]), cp(sts.at[t], s.at[at], s_s.at[t]), cp(mid.at[at], m.at[at], s_m.at[t])

        def step(k):
            j, i, t = k // CHUNKS, ring(k, CHUNKS), ring(k, FS)
            n = layer * NB + j
            rows = part(i, R)

            @when(i == 0)
            def _():
                finish(load_w(n))

                @when(n + 1 < 2 * NB)
                def _():
                    start(load_w(n + 1))

            @when(k >= FS)
            def _():
                finish(writes(k - FS))

            g[...] = nn(a[rows, :], wgu[ring(n, 2)])
            gate, up = g[:, :B], g[:, B:]
            sig = 0.5 + 0.5 * jnp.tanh(0.5 * gate)
            silu = gate * sig
            mid[rows, part(j, B)] = (silu * up).astype(bf16)
            stp[t] = up * (sig + silu * (1.0 - sig))
            sts[t] = silu
            start(writes(k))

        loop(STEPS, step)
        if layer == 0:
            load_wd.wait()
            out_a0.wait()

            def down(i):
                rows = part(i, R)
                h = (x[rows, :].astype(f32) + nn(mid[rows, :], wd[...]).astype(bf16).astype(f32)).astype(bf16)
                x[rows, :] = h
                a[rows, :] = normed(h)

            loop(CHUNKS, down)
            outs = cp(x, h1_ref, s_out.at[0]), cp(a, a1_ref, s_out.at[1])
            start(outs)
        for k in range(STEPS - FS, STEPS):
            finish(writes(k))
    finish(outs)


def forward(x, wg, wu, wd):
    states, wide, mid = (jax.ShapeDtypeStruct((T, n), t) for n, t in ((D, bf16), (FF, f32), (FF, bf16)))
    two = (2,)
    return pl.pallas_call(
        forward_kernel,
        out_shape=(states,) * 3 + (wide, wide, mid) * 2,
        in_specs=[pl.BlockSpec(memory_space=HBM)] * 4,
        out_specs=(pl.BlockSpec(memory_space=HBM),) * 9,
        scratch_shapes=[
            VMEM((T, D), bf16), VMEM((T, D), bf16), VMEM((T, FF), bf16), VMEM((2, D, 2 * B), bf16), VMEM((FF, D), bf16),
            VMEM((R, 2 * B), f32), VMEM((FS, R, B), f32), VMEM((FS, R, B), f32),
            DMA, DMA(two), DMA(two), DMA(two), DMA, DMA((FS,)), DMA((FS,)), DMA((FS,)),
        ],
        compiler_params=pltpu.CompilerParams(vmem_limit_bytes=67043328),
    )(x, wg, wu, wd)


class Reducer:
    LAGS = (0, 1, 3, 5)

    def __init__(self, source, own, out, sums, slots, total, bufs):
        self.source, self.own, self.out, self.sums, self.total = source, own, out, sums, total
        self.nx, self.ny, self.nz = slots
        (self.xr, self.ys, self.yr, self.s1, self.acc, self.zs, self.zr, self.go,
         self.xss, self.xrs, self.yss, self.yrs, self.zss, self.zrs, self.gos, self.cx, self.cy, self.cz) = bufs
        r, y, self.z, c = place()
        self.y, self.c = y, c
        self.partner, self.across = device(r, y, self.z, 1 - c), device(r, 1 - y, self.z, c)
        self.along = [device(r, y, self.zat(o), c) for o in (1, 2, 3)]

    def zat(self, o):
        return ring(self.z + o, 4)

    @staticmethod
    def scratch(shape, parts, slots):
        nx, ny, nz = slots
        return [
            VMEM((nx, 8, *shape), bf16), VMEM((ny, 4, *shape), bf16), VMEM((ny, 4, *shape), bf16), VMEM((ny, 4, *shape), f32),
            VMEM((nz, *shape), f32), VMEM((nz, 3, *shape), bf16), VMEM((nz, 3, *shape), bf16), VMEM((nz, *shape), bf16),
            DMA((nx, parts)), DMA((nx, parts)), DMA((ny,)), DMA((ny,)), DMA((nz, 3)), DMA((nz, 3)), DMA((nz,)), REGULAR, REGULAR, REGULAR((3,)),
        ]

    def copies_x(self, q):
        s = ring(q, self.nx)
        return [
            remote(src, self.xr.at[s] if b is None else self.xr.at[s, b], self.xss.at[s, b or 0], self.xrs.at[s, b or 0], self.partner)
            for src, b in self.source(q, 1 - self.c)
        ]

    def copy_y(self, q):
        s = ring(q, self.ny)
        return remote(self.ys.at[s], self.yr.at[s], self.yss.at[s], self.yrs.at[s], self.across)

    def copies_z(self, q):
        s = ring(q, self.nz)
        return [remote(self.zs.at[s, i], self.zr.at[s, 2 - i], self.zss.at[s, i], self.zrs.at[s, 2 - i], dev) for i, dev in enumerate(self.along)]

    def copy_out(self, q):
        s = ring(q, self.nz)
        return pltpu.make_async_copy(self.go.at[s], self.out(q), self.gos.at[s])

    def stage0(self, q):
        @when(q >= self.nx)
        def _():
            pl.semaphore_wait(self.cx, 1)

        start(self.copies_x(q))
        self.own.start(q)

    def stage1(self, q):
        x, s = ring(q, self.nx), ring(q, self.ny)
        self.own.wait(q)
        finish(self.copies_x(q))

        def add(i):
            b = (1 - self.y) * 4 + i
            self.ys[s, i] = (self.own.read(q, b).astype(f32) + self.xr[x, b].astype(f32)).astype(bf16)
            b = self.y * 4 + i
            self.s1[s, i] = self.own.read(q, b).astype(f32) + self.xr[x, b].astype(f32)

        loop(4, add)

        @when(q + self.nx < self.total)
        def _():
            signal(self.cx, self.partner)

        @when(q >= self.ny)
        def _():
            pl.semaphore_wait(self.cy, 1)

        self.copy_y(q).start()

    def stage2(self, q):
        s, t = ring(q, self.ny), ring(q, self.nz)
        self.copy_y(q).wait()
        for i in range(3):
            b = self.zat(i + 1)
            self.zs[t, i] = (self.s1[s, b] + self.yr[s, b].astype(f32)).astype(bf16)
        self.acc[t] = self.s1[s, self.z] + self.yr[s, self.z].astype(f32)

        @when(q + self.ny < self.total)
        def _():
            signal(self.cy, self.across)

        @when(q >= self.nz)
        def _():
            for i in range(3):
                pl.semaphore_wait(self.cz.at[i], 1)

        start(self.copies_z(q))

    def stage3(self, q):
        s = ring(q, self.nz)

        @when(q >= self.nz)
        def _():
            self.copy_out(q - self.nz).wait()

        finish(self.copies_z(q))
        total = self.acc[s]
        for i in range(3):
            total += self.zr[s, i].astype(f32)
        total = total.astype(bf16)
        self.go[s] = total
        total = total.astype(f32)
        self.sums[...] += jnp.sum((total * total).reshape(-1, 8, total.shape[-1]), 0).reshape(8, -1, 128).sum(1)

        @when(q + self.nz < self.total)
        def _():
            for i, dev in enumerate(self.along):
                signal(self.cz.at[2 - i], dev)

        self.copy_out(q).start()

    def tick(self, t, first, count):
        for i, stage in ((1, self.stage1), (0, self.stage0), (2, self.stage2), (3, self.stage3)):
            q = t - self.LAGS[i]
            when((q >= 0) & (q < count))(functools.partial(stage, first + q))

    def close(self):
        finish([self.copy_out(self.total - self.nz + i) for i in range(self.nz)])


class Staged:
    def __init__(self, at):
        self.at = at

    def start(self, q):
        pass

    wait = start

    def read(self, q, b):
        return self.at(q, b)[...]


class Fetched:
    def __init__(self, source, buf, sems, slots):
        self.source, self.buf, self.sems, self.slots = source, buf, sems, slots

    def copies(self, q):
        s = ring(q, self.slots)
        return [pltpu.make_async_copy(src, self.buf.at[s, b], self.sems.at[s, b]) for src, b in self.source(q)]

    def start(self, q):
        start(self.copies(q))

    def wait(self, q):
        finish(self.copies(q))

    def read(self, q, b):
        return self.buf[ring(q, self.slots), b]


DC, DP = 256, 4
GP = 2 * NB
HALF = 512
GS, DS = (2, 3, 3), (2, 3, 3)
MS = 3
ES = 3
ROWS = B // 8


def backward_kernel(
    dy_ref, h1_ref, a1_ref, a0_ref, p1, s1, mid1, p0, s0, mid0, wg_ref, wu_ref, wd_ref,
    g_out, d_out, sums_out, dd_ref,
    sums, dh, a, da, pa, sa, dgu, wgu, wdj, dwst, ddst, xo,
    tot, got, s_tot, s_tot_in, s_dh, s_a, s_ps, s_mid, s_wgu, s_wd, s_dd, s_xo, *bufs,
):
    half = len(bufs) // 2
    r, y, z, c = place()
    cp = pltpu.make_async_copy

    load_dh = cp(dy_ref, dh, s_dh)
    load_a = cp(a1_ref, a, s_a)
    load_h, load_a0 = cp(h1_ref, a, s_a), cp(a0_ref, a, s_a)
    load_dh.start()
    greet(r, y, z, c)
    sums[...] = jnp.zeros_like(sums)
    da[...] = jnp.zeros_like(da)

    def g_part(q):
        return ring(q // 2, 2), part(ring(q, 2), B)

    def g_source(q, c):
        s, cols = g_part(q)
        return [(dwst.at[s, :, c, :, cols], None)]

    def g_own(q, b):
        s, cols = g_part(q)
        return dwst.at[s, b, c, :, cols]

    def g_to(q):
        n = q // 2
        return g_out.at[ring(q, 2), 1 - n // NB, :, part(ring(n, NB), B)]

    def d_source(q, c):
        return [(dd_ref.at[q // DP, pl.ds((2 * b + c) * 25, 25), :, part(ring(q, DP), DC)], b) for b in range(8)]

    def d_to(q):
        return d_out.at[1 - q // DP, :, :, part(ring(q, DP), DC)]

    gr = Reducer(g_source, Staged(g_own), g_to, sums, GS, 2 * GP, bufs[:half])
    dr = Reducer(d_source, Fetched(lambda q: d_source(q, c), xo, s_xo, DS[0]), d_to, sums, DS, 2 * DP, bufs[half:])

    for n, (p, s, mid) in enumerate(((p1, s1, mid1), (p0, s0, mid0))):
        layer, d_first, g_first = 1 - n, n * DP, n * GP

        def load_mid(st):
            t = ring(st, MS)
            return cp(mid.at[:, part(ring(st, NB), B)], dgu.at[:, part(t, B)], s_mid.at[t])

        def write_dd(i, h, t):
            return cp(ddst.at[t], dd_ref.at[n, part(i, ROWS), :, part(h, HALF)], s_dd.at[t])

        def load_wd(j):
            return cp(wd_ref.at[layer, part(j, B)], wdj, s_wd)

        def load_wgu(j):
            return [cp(w.at[layer, :, part(j, B)], wgu.at[:, part(i, B)], s_wgu.at[i]) for i, w in enumerate((wg_ref, wu_ref))]

        def load_ps(k):
            t, at = ring(k, ES), (part(ring(k, CHUNKS), R), part(k // CHUNKS, B))
            return cp(p.at[at], pa.at[t], s_ps.at[t, 0]), cp(s.at[at], sa.at[t], s_ps.at[t, 1])

        def first_loads():
            load_wd(0).start()
            for k in range(ES - 1):
                start(load_ps(k))

        for k in range(MS - 1):
            load_mid(k).start()
        if n == 0:
            load_dh.wait()
        else:

            def norm(i):
                rows = part(i, N)
                wide = a[rows, :].astype(f32)
                d = da[rows, :].astype(bf16).astype(f32)
                scale = lax.rsqrt(jnp.mean(wide * wide, -1, keepdims=True) + 1e-6)
                inner = jnp.mean(d * wide, -1, keepdims=True)
                dn = (scale * d - wide * (scale * scale * scale * inner)).astype(bf16)
                dh[rows, :] = (dh[rows, :].astype(f32) + dn.astype(f32)).astype(bf16)

            load_h.wait()
            loop(T // N, norm)

        def tile(t, st, h):
            ddst[t] = tn(dgu[:, part(ring(st, MS), B)], dh[:, part(h, HALF)]).astype(bf16).reshape(ROWS, 8, HALF)

        def down(st):
            @when(st + MS - 1 < 2 * NB)
            def _():
                load_mid(st + MS - 1).start()

            @when(st == 1)
            def _():
                (load_a0 if n else load_a).start()
                first_loads()

            load_mid(st).wait()
            t, i, h = ring(st, 2), ring(st, NB), st // NB
            tile(t, st, h)

            @when((st != 0) & (st != NB))
            def _():
                write_dd(ring(st - 1, NB), h, 1 - t).wait()

            write_dd(i, h, t).start()

            @when(i == NB - 1)
            def _():
                write_dd(i, h, t).wait()

            @when((st == 4) | (st == 6) | (st == 9))
            def _():
                dr.tick((st - 4) // 2, d_first, DP)

            if n:

                @when((st == 0) | (st == 2) | (st == 5) | (st == 7) | (st == 9))
                def _():
                    gr.tick(GP + st // 2, 0, GP)

        loop(2 * NB, down)
        (load_a0 if n else load_a).wait()

        def block(j):
            if n == 0:
                start(load_wgu(j))
            load_wd(j).wait()

            def dmids(i):
                k, rows = j * CHUNKS + i, part(i, R)
                t = ring(k, ES)

                @when(k + ES - 1 < NB * CHUNKS)
                def _():
                    start(load_ps(k + ES - 1))

                finish(load_ps(k))
                dm = nt(dh[rows, :], wdj[...]).astype(bf16).astype(f32)
                dgu[rows, :B] = (dm * pa[t]).astype(bf16)
                dgu[rows, B : 2 * B] = (dm * sa[t]).astype(bf16)

            loop(CHUNKS, dmids)

            @when(j + 1 < NB)
            def _():
                load_wd(j + 1).start()

            dr.tick(3 + 2 * j, d_first, DP)

            @when(j >= 1)
            def _():
                gr.tick(2 * j - 1, g_first, GP)

            def terms(i):
                dwst[ring(n * NB + j, 2), part(i, 4)] = tn(a[:, part(i, R)], dgu[:, : 2 * B]).astype(bf16).reshape(4, 2, 64, 2 * B)

            loop(D // R, terms)

            dr.tick(4 + 2 * j, d_first, DP)
            gr.tick(2 * j, g_first, GP)

            if n == 0:

                @when(j == NB - 1)
                def _():
                    load_h.start()

                finish(load_wgu(j))

                def back(i):
                    rows = part(i, R)
                    da[rows, :] += nt(dgu[rows, : 2 * B], wgu[...])

                loop(CHUNKS, back)

        loop(NB, block)
        gr.tick(GP - 1, g_first, GP)
    loop(NB, lambda t: gr.tick(GP + t, GP, GP))
    dr.close()
    gr.close()

    tot[0] = sums[...]
    for i, dev in enumerate((gr.partner, gr.across)):
        copy = remote(tot.at[i], got.at[i], s_tot.at[i], s_tot_in.at[i], dev)
        copy.start()
        copy.wait()
        tot[i + 1] = tot[i] + got[i]
    copies = [remote(tot.at[2], got.at[2 + z], s_tot.at[2 + i], s_tot_in.at[4 - i], dev) for i, dev in enumerate(gr.along)]
    start(copies)
    finish(copies)
    got[2 + z] = tot[2]
    sums_out[...] = got[2] + got[3] + got[4] + got[5]


def backward(*arrays):
    return pl.pallas_call(
        backward_kernel,
        out_shape=(
            jax.ShapeDtypeStruct((2, 2, 64, FF), bf16),
            jax.ShapeDtypeStruct((2, 25, 8, D), bf16),
            jax.ShapeDtypeStruct((8, 128), f32),
            jax.ShapeDtypeStruct((2, FF // 8, 8, D), bf16),
        ),
        in_specs=[pl.BlockSpec(memory_space=HBM)] * len(arrays),
        out_specs=tuple(pl.BlockSpec(memory_space=m) for m in (HBM, HBM, VMEM, HBM)),
        scratch_shapes=[
            VMEM((8, 128), f32), VMEM((T, D), bf16), VMEM((T, D), bf16), VMEM((T, D), f32), VMEM((ES, R, B), f32), VMEM((ES, R, B), f32),
            VMEM((T, MS * B), bf16), VMEM((D, 2 * B), bf16), VMEM((B, D), bf16), VMEM((2, 8, 2, 64, 2 * B), bf16),
            VMEM((2, ROWS, 8, HALF), bf16), VMEM((DS[0], 8, 25, 8, DC), bf16),
            VMEM((3, 8, 128), f32), VMEM((6, 8, 128), f32), DMA((5,)), DMA((5,)),
            DMA, DMA, DMA((ES, 2)), DMA((MS,)), DMA((2,)), DMA, DMA((2,)), DMA((DS[0], 8)),
        ] + Reducer.scratch((64, B), 1, GS) + Reducer.scratch((25, 8, DC), 8, DS),
        compiler_params=pltpu.CompilerParams(collective_id=0, has_side_effects=True, vmem_limit_bytes=67043328),
    )(*arrays)


def gather_kernel(sg, su, sd, og, ou, od, zss, zrs, yss, yrs, dss, drs, ls):
    r, y, z, c = place()
    greet(r, y, z, c)
    chunks = [(s, o, layer) for layer in range(2) for s, o in ((sg, og), (su, ou), (sd, od))]
    last = len(chunks) - 1
    entries = [(k, y) for k in range(last + 1)] + [(last, 1 - y)]
    partner, across = device(r, y, z, 1 - c), device(r, 1 - y, z, c)
    beside = device(r, y, ring(z + 1, 4), c), device(r, y, ring(z + 3, 4), c)
    sides = range(2)
    goes_on = z < 3, z > 0

    def there(d, side):
        return z + d <= 3 if side else z >= d

    def at(d, side):
        return z + d if side else z - d

    def block(k, row, zz, c=c):
        return chunks[k][1].at[chunks[k][2], row * 8 + zz * 2 + c]

    def along(src, e, zz, d, side):
        k, row = entries[e]
        when(goes_on[side])(remote(src, block(k, row, zz), zss.at[e, d - 1, side], zrs.at[e, d - 1, side], beside[side]).start)

    def over(src, k, zz, w):
        remote(src, block(k, y, zz), yss.at[k, w], yrs.at[k, w], across).start()

    def pair(src, k, row, zz):
        remote(src, block(k, row, zz), dss.at[k, row * 4 + zz], drs.at[k, row * 4 + zz], partner).start()

    def arrived(ref, sem):
        remote(ref, ref, sem, sem, partner).wait_recv()
        return ref

    def left(ref, sem):
        remote(ref, ref, sem, sem, partner).wait_send()

    def which(d, side):
        return 2 * d - 1 + side

    own = [s.at[layer] for s, _, layer in chunks]
    for k in [last, *range(last)]:
        over(own[k], k, z, 0)
    kept = [pltpu.make_async_copy(src, block(k, y, z), ls.at[k]) for k, src in enumerate(own)]
    for k, src in enumerate(own):
        for side in sides:
            along(src, k, z, 1, side)
        pair(src, k, y, z)
        kept[k].start()
    src = arrived(block(last, 1 - y, z), yrs.at[last, 0])
    for side in sides:
        along(src, last + 1, z, 1, side)
    pair(src, last, 1 - y, z)

    def crossed(d, k):
        for side in sides[: 1 + min(d, 1)]:

            def hand(zz, w):
                pair(arrived(block(k, 1 - y, zz), yrs.at[k, w]), k, 1 - y, zz)

            if d:
                when(there(d, side))(functools.partial(hand, at(d, side), which(d, side)))
            else:
                hand(z, 0)

    for d in (1, 2, 3):
        for e, (k, row) in enumerate(entries):
            for side in sides:

                @when(there(d, side))
                def _():
                    zz = at(d, side)
                    src = arrived(block(k, row, zz), zrs.at[e, d - 1, side])
                    if d < 3:
                        along(src, e, zz, d + 1, side)
                    if k != last:
                        over(src, k, zz, which(d, side))
                    pair(src, k, row, zz)

            if k != last:
                crossed(d - 1, k)
    for k in range(last):
        crossed(3, k)

    for k in range(last + 1):
        for b in range(8):
            left(arrived(block(k, 0, b, 1 - c), drs.at[k, b]), dss.at[k, b])
        left(own[k], yss.at[k, 0])
    for d in range(3):
        for side in sides:
            for e in range(len(entries)):
                when(goes_on[side] & there(d, side))(functools.partial(left, own[entries[e][0]], zss.at[e, d, side]))
            for k in range(last):
                when(there(d + 1, side))(functools.partial(left, own[k], yss.at[k, which(d + 1, side)]))
    finish(kept)


def all_gather(*shards):
    out = pl.pallas_call(
        gather_kernel,
        out_shape=[jax.ShapeDtypeStruct((2, 16, *s.shape[1:]), bf16) for s in shards],
        in_specs=[pl.BlockSpec(memory_space=HBM)] * 3,
        out_specs=[pl.BlockSpec(memory_space=pl.ANY)] * 3,
        scratch_shapes=[DMA((7, 3, 2)), DMA((7, 3, 2)), DMA((6, 7)), DMA((6, 7)), DMA((6, 8)), DMA((6, 8)), DMA((6,))],
        compiler_params=pltpu.CompilerParams(collective_id=1, has_side_effects=True, vmem_limit_bytes=2**23),
    )(*shards)
    return [o.reshape(2, -1, o.shape[-1]) for o in out]


def adamw(w, m, v, g):
    m = 0.9 * m + 0.1 * g
    v = 0.95 * v + 0.05 * g * g
    step = m * lax.rsqrt(v + 1e-8) + 0.1 * w
    return (w - 0.02 * step).astype(bf16), m, v


def solution(mesh):
    def step(x, dy, wg, wu, wd, mg, mu, md, vg, vu, vd):
        a0, a1, h1, p0, s0, mid0, p1, s1, mid1 = forward(x[0], wg, wu, wd)
        gg, gd, sums, _ = backward(dy[0], h1, a1, a0, p1, s1, mid1, p0, s0, mid0, wg, wu, wd)
        factor = jnp.minimum(1.0, 0.5 * lax.rsqrt(jnp.sum(sums) / (6 * D * FF) + 1e-30))
        me = lax.axis_index("dp")
        new = []
        for w, m, v, g in ((wg, mg, vg, gg[0]), (wu, mu, vu, gg[1]), (wd, md, vd, gd.reshape(2, 200, D))):
            rows = m.shape[1]
            mine = lax.dynamic_slice_in_dim(w, me * rows, rows, 1)
            new.append(adamw(mine.astype(f32), m, v, g.astype(f32) * factor))
        weights = all_gather(*(n[0] for n in new))
        return (*weights, *(n[1] for n in new), *(n[2] for n in new))

    seq, rep, own = P(("rep", "dp")), P("rep"), P("rep", "dp")
    return jax.shard_map(
        step,
        mesh=mesh,
        in_specs=(seq, seq, P(), P(), P(), *[P(None, "dp")] * 6),
        out_specs=(rep,) * 3 + (own,) * 6,
        check_vma=False,
    )
```

```python
import functools

import jax
import jax.numpy as jnp
from jax import lax
from jax.experimental import pallas as pl
from jax.experimental.pallas import tpu as pltpu
from jax.sharding import PartitionSpec as P

MESH = pl.DeviceIdType.MESH
HBM, VMEM = pltpu.HBM, pltpu.VMEM
DMA, REGULAR = pltpu.SemaphoreType.DMA, pltpu.SemaphoreType.REGULAR
bf16, f32 = jnp.bfloat16, jnp.float32
D, FF, T = 1024, 3200, 2048
B = 640
NB = FF // B
R = 512
ring = lax.rem


def place():
    me = lax.axis_index("dp")
    return lax.axis_index("rep"), me // 8, ring(me // 2, 4), ring(me, 2)


def device(r, y, z, c):
    return (r, y * 8 + z * 2 + c)


def greet(r, y, z, c, *more):
    bar = pltpu.get_barrier_semaphore()
    peers = [device(r, y, z, 1 - c), device(r, 1 - y, z, c)] + [device(r, y, ring(z + o, 4), c) for o in (1, 2, 3)] + list(more)
    for p in peers:
        signal(bar, p)
    pl.semaphore_wait(bar, len(peers))


def signal(sem, dev):
    pl.semaphore_signal(sem, 1, device_id=dev, device_id_type=MESH)


def remote(src, dst, ssem, rsem, dev):
    return pltpu.make_async_remote_copy(src, dst, ssem, rsem, device_id=dev, device_id_type=MESH)


def start(copies):
    for copy in copies:
        copy.start()


def finish(copies):
    for copy in copies:
        copy.wait()


def loop(n, body):
    lax.fori_loop(0, n, lambda i, carry: (body(i), carry)[1], None)


def when(ok):
    return pl.when(ok)


def part(i, n):
    return pl.ds(pl.multiple_of(i * n, n), n)


def dot(a, b, ca, cb):
    return lax.dot_general(a, b, (((ca,), (cb,)), ((), ())), preferred_element_type=f32)


nn = functools.partial(dot, ca=1, cb=0)
nt = functools.partial(dot, ca=1, cb=1)
tn = functools.partial(dot, ca=0, cb=0)


def normed(h):
    wide = h.astype(f32)
    return (wide * lax.rsqrt(jnp.mean(wide * wide, -1, keepdims=True) + 1e-6)).astype(bf16)


N = 128
CHUNKS = T // R
STEPS = NB * CHUNKS
FS = 4


def forward_kernel(
    x_ref, wg_ref, wu_ref, wd_ref,
    a0_ref, a1_ref, h1_ref, p0, s0, m0, p1, s1, m1,
    x, a, mid, wgu, wd, g, stp, sts, s_x, s_out, s_wg, s_wu, s_wd, s_p, s_s, s_m,
):
    cp = pltpu.make_async_copy

    def load_w(n):
        s, cols = ring(n, 2), part(ring(n, NB), B)
        return (cp(wg_ref.at[n // NB, :, cols], wgu.at[s, :, pl.ds(0, B)], s_wg.at[s]),
                cp(wu_ref.at[n // NB, :, cols], wgu.at[s, :, pl.ds(B, B)], s_wu.at[s]))

    load_x, load_wd = cp(x_ref, x, s_x), cp(wd_ref.at[0], wd, s_wd)
    load_x.start()
    start(load_w(0))
    load_wd.start()
    load_x.wait()

    def norm(i):
        rows = part(i, N)
        a[rows, :] = normed(x[rows, :])

    loop(T // N, norm)
    out_a0 = cp(a, a0_ref, s_out.at[0])
    out_a0.start()
    for layer, (p, s, m) in enumerate(((p0, s0, m0), (p1, s1, m1))):

        def writes(k):
            t, at = ring(k, FS), (part(ring(k, CHUNKS), R), part(k // CHUNKS, B))
            return cp(stp.at[t], p.at[at], s_p.at[t]), cp(sts.at[t], s.at[at], s_s.at[t]), cp(mid.at[at], m.at[at], s_m.at[t])

        def step(k):
            j, i, t = k // CHUNKS, ring(k, CHUNKS), ring(k, FS)
            n = layer * NB + j
            rows = part(i, R)

            @when(i == 0)
            def _():
                finish(load_w(n))

                @when(n + 1 < 2 * NB)
                def _():
                    start(load_w(n + 1))

            @when(k >= FS)
            def _():
                finish(writes(k - FS))

            g[...] = nn(a[rows, :], wgu[ring(n, 2)])
            gate, up = g[:, :B], g[:, B:]
            sig = 0.5 + 0.5 * jnp.tanh(0.5 * gate)
            silu = gate * sig
            mid[rows, part(j, B)] = (silu * up).astype(bf16)
            stp[t] = up * (sig + silu * (1.0 - sig))
            sts[t] = silu
            start(writes(k))

        loop(STEPS, step)
        if layer == 0:
            load_wd.wait()
            out_a0.wait()

            def down(i):
                rows = part(i, R)
                h = (x[rows, :].astype(f32) + nn(mid[rows, :], wd[...]).astype(bf16).astype(f32)).astype(bf16)
                x[rows, :] = h
                a[rows, :] = normed(h)

            loop(CHUNKS, down)
            outs = cp(x, h1_ref, s_out.at[0]), cp(a, a1_ref, s_out.at[1])
            start(outs)
        for k in range(STEPS - FS, STEPS):
            finish(writes(k))
    finish(outs)


def forward(x, wg, wu, wd):
    states, wide, mid = (jax.ShapeDtypeStruct((T, n), t) for n, t in ((D, bf16), (FF, f32), (FF, bf16)))
    two = (2,)
    return pl.pallas_call(
        forward_kernel,
        out_shape=(states,) * 3 + (wide, wide, mid) * 2,
        in_specs=[pl.BlockSpec(memory_space=HBM)] * 4,
        out_specs=(pl.BlockSpec(memory_space=HBM),) * 9,
        scratch_shapes=[
            VMEM((T, D), bf16), VMEM((T, D), bf16), VMEM((T, FF), bf16), VMEM((2, D, 2 * B), bf16), VMEM((FF, D), bf16),
            VMEM((R, 2 * B), f32), VMEM((FS, R, B), f32), VMEM((FS, R, B), f32),
            DMA, DMA(two), DMA(two), DMA(two), DMA, DMA((FS,)), DMA((FS,)), DMA((FS,)),
        ],
        compiler_params=pltpu.CompilerParams(vmem_limit_bytes=67043328),
    )(x, wg, wu, wd)


class Reducer:
    LAGS = (0, 1, 3, 5)

    def __init__(self, source, own, out, sums, slots, total, bufs):
        self.source, self.own, self.out, self.sums, self.total = source, own, out, sums, total
        self.nx, self.ny, self.nz = slots
        (self.xr, self.ys, self.yr, self.s1, self.acc, self.zs, self.zr, self.go,
         self.xss, self.xrs, self.yss, self.yrs, self.zss, self.zrs, self.gos, self.cx, self.cy, self.cz) = bufs
        r, y, self.z, c = place()
        self.y, self.c = y, c
        self.partner, self.across = device(r, y, self.z, 1 - c), device(r, 1 - y, self.z, c)
        self.along = [device(r, y, self.zat(o), c) for o in (1, 2, 3)]

    def zat(self, o):
        return ring(self.z + o, 4)

    @staticmethod
    def scratch(shape, parts, slots):
        nx, ny, nz = slots
        return [
            VMEM((nx, 8, *shape), bf16), VMEM((ny, 4, *shape), bf16), VMEM((ny, 4, *shape), bf16), VMEM((ny, 4, *shape), f32),
            VMEM((nz, *shape), f32), VMEM((nz, 3, *shape), bf16), VMEM((nz, 3, *shape), bf16), VMEM((nz, *shape), bf16),
            DMA((nx, parts)), DMA((nx, parts)), DMA((ny,)), DMA((ny,)), DMA((nz, 3)), DMA((nz, 3)), DMA((nz,)), REGULAR, REGULAR, REGULAR((3,)),
        ]

    def copies_x(self, q):
        s = ring(q, self.nx)
        return [
            remote(src, self.xr.at[s] if b is None else self.xr.at[s, b], self.xss.at[s, b or 0], self.xrs.at[s, b or 0], self.partner)
            for src, b in self.source(q, 1 - self.c)
        ]

    def copy_y(self, q):
        s = ring(q, self.ny)
        return remote(self.ys.at[s], self.yr.at[s], self.yss.at[s], self.yrs.at[s], self.across)

    def copies_z(self, q):
        s = ring(q, self.nz)
        return [remote(self.zs.at[s, i], self.zr.at[s, 2 - i], self.zss.at[s, i], self.zrs.at[s, 2 - i], dev) for i, dev in enumerate(self.along)]

    def copy_out(self, q):
        s = ring(q, self.nz)
        return pltpu.make_async_copy(self.go.at[s], self.out(q), self.gos.at[s])

    def stage0(self, q):
        @when(q >= self.nx)
        def _():
            pl.semaphore_wait(self.cx, 1)

        start(self.copies_x(q))
        self.own.start(q)

    def stage1(self, q):
        x, s = ring(q, self.nx), ring(q, self.ny)
        self.own.wait(q)
        finish(self.copies_x(q))

        def add(i):
            b = (1 - self.y) * 4 + i
            self.ys[s, i] = (self.own.read(q, b).astype(f32) + self.xr[x, b].astype(f32)).astype(bf16)
            b = self.y * 4 + i
            self.s1[s, i] = self.own.read(q, b).astype(f32) + self.xr[x, b].astype(f32)

        loop(4, add)

        @when(q + self.nx < self.total)
        def _():
            signal(self.cx, self.partner)

        @when(q >= self.ny)
        def _():
            pl.semaphore_wait(self.cy, 1)

        self.copy_y(q).start()

    def stage2(self, q):
        s, t = ring(q, self.ny), ring(q, self.nz)
        self.copy_y(q).wait()
        for i in range(3):
            b = self.zat(i + 1)
            self.zs[t, i] = (self.s1[s, b] + self.yr[s, b].astype(f32)).astype(bf16)
        self.acc[t] = self.s1[s, self.z] + self.yr[s, self.z].astype(f32)

        @when(q + self.ny < self.total)
        def _():
            signal(self.cy, self.across)

        @when(q >= self.nz)
        def _():
            for i in range(3):
                pl.semaphore_wait(self.cz.at[i], 1)

        start(self.copies_z(q))

    def stage3(self, q):
        s = ring(q, self.nz)

        @when(q >= self.nz)
        def _():
            self.copy_out(q - self.nz).wait()

        finish(self.copies_z(q))
        total = self.acc[s]
        for i in range(3):
            total += self.zr[s, i].astype(f32)
        total = total.astype(bf16)
        self.go[s] = total
        total = total.astype(f32)
        self.sums[...] += jnp.sum((total * total).reshape(-1, 8, total.shape[-1]), 0).reshape(8, -1, 128).sum(1)

        @when(q + self.nz < self.total)
        def _():
            for i, dev in enumerate(self.along):
                signal(self.cz.at[2 - i], dev)

        self.copy_out(q).start()

    def tick(self, t, first, count):
        for i, stage in ((1, self.stage1), (0, self.stage0), (2, self.stage2), (3, self.stage3)):
            q = t - self.LAGS[i]
            when((q >= 0) & (q < count))(functools.partial(stage, first + q))

    def run(self, stages, first):
        for stage, q in stages:
            (self.stage0, self.stage1, self.stage2, self.stage3)[stage](first + q)

    def close(self):
        finish([self.copy_out(self.total - self.nz + i) for i in range(self.nz)])


class Staged:
    def __init__(self, at):
        self.at = at

    def start(self, q):
        pass

    wait = start

    def read(self, q, b):
        return self.at(q, b)[...]


class Fetched:
    def __init__(self, source, buf, sems, slots):
        self.source, self.buf, self.sems, self.slots = source, buf, sems, slots

    def copies(self, q):
        s = ring(q, self.slots)
        return [pltpu.make_async_copy(src, self.buf.at[s, b], self.sems.at[s, b]) for src, b in self.source(q)]

    def start(self, q):
        start(self.copies(q))

    def wait(self, q):
        finish(self.copies(q))

    def read(self, q, b):
        return self.buf[ring(q, self.slots), b]


DC, DP = 256, 4
GP = 2 * NB
HALF = 512
GS, DS = (2, 3, 3), (2, 3, 3)
MS = 3
ES = 3
ROWS = B // 8


STAGES = (
    ((4, ((0, 0), (0, 1))), (6, ((1, 0), (1, 1))), (9, ((0, 2), (0, 3), (2, 0)))),
    ((0, ((1, 2), (1, 3), (2, 1))), (1, ((2, 3), (3, 1))), (2, ((3, 3),))),
    ((0, ((2, 2), (3, 0))), (1, ((3, 2),))),
)


def backward_kernel(
    dy_ref, h1_ref, a1_ref, a0_ref, p1, s1, mid1, p0, s0, mid0, wg_ref, wu_ref, wd_ref,
    g_out, d_out, sums_out, dd_ref,
    sums, dh, a, da, pa, sa, dgu, wgu, wdj, dwst, ddst, xo,
    tot, got, s_tot, s_tot_in, s_dh, s_a, s_ps, s_mid, s_wgu, s_wd, s_dd, s_xo, *bufs,
):
    half = len(bufs) // 2
    r, y, z, c = place()
    cp = pltpu.make_async_copy

    load_dh = cp(dy_ref, dh, s_dh)
    load_a = cp(a1_ref, a, s_a)
    load_h, load_a0 = cp(h1_ref, a, s_a), cp(a0_ref, a, s_a)
    load_dh.start()

    def g_part(q):
        return ring(q // 2, 2), part(ring(q, 2), B)

    def g_source(q, c):
        s, cols = g_part(q)
        return [(dwst.at[s, :, c, :, cols], None)]

    def g_own(q, b):
        s, cols = g_part(q)
        return dwst.at[s, b, c, :, cols]

    def g_to(q):
        n = q // 2
        return g_out.at[ring(q, 2), 1 - n // NB, :, part(ring(n, NB), B)]

    def d_source(q, c):
        return [(dd_ref.at[q // DP, pl.ds((2 * b + c) * 25, 25), :, part(ring(q, DP), DC)], b) for b in range(8)]

    def d_to(q):
        return d_out.at[1 - q // DP, :, :, part(ring(q, DP), DC)]

    gr = Reducer(g_source, Staged(g_own), g_to, sums, GS, 2 * GP, bufs[:half])
    dr = Reducer(d_source, Fetched(lambda q: d_source(q, c), xo, s_xo, DS[0]), d_to, sums, DS, 2 * DP, bufs[half:])

    for n, (p, s, mid) in enumerate(((p1, s1, mid1), (p0, s0, mid0))):
        layer, d_first, g_first = 1 - n, n * DP, n * GP

        def load_mid(st):
            t = ring(st, MS)
            return cp(mid.at[:, part(ring(st, NB), B)], dgu.at[:, part(t, B)], s_mid.at[t])

        def write_dd(i, h, t):
            return cp(ddst.at[t], dd_ref.at[n, part(i, ROWS), :, part(h, HALF)], s_dd.at[t])

        def load_wd(j):
            return cp(wd_ref.at[layer, part(j, B)], wdj, s_wd)

        def load_wgu(j):
            return [cp(w.at[layer, :, part(j, B)], wgu.at[:, part(i, B)], s_wgu.at[i]) for i, w in enumerate((wg_ref, wu_ref))]

        def load_ps(k):
            t, at = ring(k, ES), (part(ring(k, CHUNKS), R), part(k // CHUNKS, B))
            return cp(p.at[at], pa.at[t], s_ps.at[t, 0]), cp(s.at[at], sa.at[t], s_ps.at[t, 1])

        def first_loads():
            load_wd(0).start()
            for k in range(ES - 1):
                start(load_ps(k))

        for k in range(MS - 1):
            load_mid(k).start()
        if n == 0:
            sums[...] = jnp.zeros_like(sums)
            da[...] = jnp.zeros_like(da)
            greet(r, y, z, c, device(r, 1 - y, z, 1 - c))
            load_dh.wait()
        else:

            def norm(i):
                rows = part(i, N)
                wide = a[rows, :].astype(f32)
                d = da[rows, :].astype(bf16).astype(f32)
                scale = lax.rsqrt(jnp.mean(wide * wide, -1, keepdims=True) + 1e-6)
                inner = jnp.mean(d * wide, -1, keepdims=True)
                dn = (scale * d - wide * (scale * scale * scale * inner)).astype(bf16)
                dh[rows, :] = (dh[rows, :].astype(f32) + dn.astype(f32)).astype(bf16)

            load_h.wait()
            loop(T // N, norm)

        def down_pieces(where, i):
            if n:
                for at, stages in STAGES[where]:
                    when(i == at)(functools.partial(dr.run, stages, d_first))
            elif where:
                dr.tick(2 + where + 2 * i, d_first, DP)
            else:
                when((i == 4) | (i == 6) | (i == 9))(lambda: dr.tick((i - 4) // 2, d_first, DP))

        def tile(t, st, h):
            ddst[t] = tn(dgu[:, part(ring(st, MS), B)], dh[:, part(h, HALF)]).astype(bf16).reshape(ROWS, 8, HALF)

        def down(st):
            @when(st + MS - 1 < 2 * NB)
            def _():
                load_mid(st + MS - 1).start()

            when(st == 4)(first_loads)
            when(st == 6)((load_a0 if n else load_a).start)

            load_mid(st).wait()
            t, i, h = ring(st, 2), ring(st, NB), st // NB
            tile(t, st, h)

            @when((st != 0) & (st != NB))
            def _():
                write_dd(ring(st - 1, NB), h, 1 - t).wait()

            write_dd(i, h, t).start()

            @when(i == NB - 1)
            def _():
                write_dd(i, h, t).wait()

            down_pieces(0, st)

            if n:

                for i, at in enumerate((0, 4, 6, 8, 9)):
                    when(st == at)(functools.partial(gr.tick, GP + i, 0, GP))

        loop(2 * NB, down)
        (load_a0 if n else load_a).wait()

        def block(j):
            if n == 0:
                start(load_wgu(j))
            load_wd(j).wait()

            def dmids(i):
                k, rows = j * CHUNKS + i, part(i, R)
                t = ring(k, ES)

                @when(k + ES - 1 < NB * CHUNKS)
                def _():
                    start(load_ps(k + ES - 1))

                finish(load_ps(k))
                dm = nt(dh[rows, :], wdj[...]).astype(bf16).astype(f32)
                dgu[rows, :B] = (dm * pa[t]).astype(bf16)
                dgu[rows, B : 2 * B] = (dm * sa[t]).astype(bf16)

            loop(CHUNKS, dmids)

            @when(j + 1 < NB)
            def _():
                load_wd(j + 1).start()

            down_pieces(1, j)

            @when(j >= 1)
            def _():
                gr.tick(2 * j - 1, g_first, GP)

            def terms(i):
                dwst[ring(n * NB + j, 2), part(i, 4)] = tn(a[:, part(i, R)], dgu[:, : 2 * B]).astype(bf16).reshape(4, 2, 64, 2 * B)

            loop(D // R, terms)

            down_pieces(2, j)
            gr.tick(2 * j, g_first, GP)

            if n == 0:

                @when(j == NB - 1)
                def _():
                    load_h.start()

                finish(load_wgu(j))

                def back(i):
                    rows = part(i, R)
                    da[rows, :] += nt(dgu[rows, : 2 * B], wgu[...])

                loop(CHUNKS, back)

        loop(NB, block)
        gr.tick(GP - 1, g_first, GP)
    loop(NB, lambda t: gr.tick(GP + t, GP, GP))
    def swap(src, at, devs, sems):
        copies = [remote(src, got.at[at], s_tot.at[send], s_tot_in.at[recv], dev) for (send, recv), dev in zip(sems, devs, strict=True)]
        start(copies)
        got[at] = src[...]
        finish(copies)

    swap(sums, y * 2 + c, (gr.partner, gr.across, device(r, 1 - y, z, 1 - c)), ((0, 0), (1, 1), (2, 2)))
    tot[...] = got[0] + got[1] + got[2] + got[3]
    swap(tot, 4 + z, gr.along, ((3, 5), (4, 4), (5, 3)))
    sums_out[...] = got[4] + got[5] + got[6] + got[7]
    dr.close()
    gr.close()


def backward(*arrays):
    return pl.pallas_call(
        backward_kernel,
        out_shape=(
            jax.ShapeDtypeStruct((2, 2, 64, FF), bf16),
            jax.ShapeDtypeStruct((2, 25, 8, D), bf16),
            jax.ShapeDtypeStruct((8, 128), f32),
            jax.ShapeDtypeStruct((2, FF // 8, 8, D), bf16),
        ),
        in_specs=[pl.BlockSpec(memory_space=HBM)] * len(arrays),
        out_specs=tuple(pl.BlockSpec(memory_space=m) for m in (HBM, HBM, VMEM, HBM)),
        scratch_shapes=[
            VMEM((8, 128), f32), VMEM((T, D), bf16), VMEM((T, D), bf16), VMEM((T, D), f32), VMEM((ES, R, B), f32), VMEM((ES, R, B), f32),
            VMEM((T, MS * B), bf16), VMEM((D, 2 * B), bf16), VMEM((B, D), bf16), VMEM((2, 8, 2, 64, 2 * B), bf16),
            VMEM((2, ROWS, 8, HALF), bf16), VMEM((DS[0], 8, 25, 8, DC), bf16),
            VMEM((8, 128), f32), VMEM((8, 8, 128), f32), DMA((6,)), DMA((6,)),
            DMA, DMA, DMA((ES, 2)), DMA((MS,)), DMA((2,)), DMA, DMA((2,)), DMA((DS[0], 8)),
        ] + Reducer.scratch((64, B), 1, GS) + Reducer.scratch((25, 8, DC), 8, DS),
        compiler_params=pltpu.CompilerParams(collective_id=0, has_side_effects=True, vmem_limit_bytes=67043328),
    )(*arrays)


def gather_kernel(sg, su, sd, og, ou, od, zss, zrs, yss, yrs, dss, drs, ls):
    r, y, z, c = place()
    greet(r, y, z, c)
    chunks = [(s, o, layer) for layer in range(2) for s, o in ((sg, og), (su, ou), (sd, od))]
    last = len(chunks) - 1
    entries = [(k, y) for k in range(last + 1)] + [(last, 1 - y)]
    partner, across = device(r, y, z, 1 - c), device(r, 1 - y, z, c)
    beside = device(r, y, ring(z + 1, 4), c), device(r, y, ring(z + 3, 4), c)
    sides = range(2)
    goes_on = z < 3, z > 0

    def there(d, side):
        return z + d <= 3 if side else z >= d

    def at(d, side):
        return z + d if side else z - d

    def block(k, row, zz, c=c):
        return chunks[k][1].at[chunks[k][2], row * 8 + zz * 2 + c]

    def along(src, e, zz, d, side):
        k, row = entries[e]
        when(goes_on[side])(remote(src, block(k, row, zz), zss.at[e, d - 1, side], zrs.at[e, d - 1, side], beside[side]).start)

    def over(src, k, zz, w):
        remote(src, block(k, y, zz), yss.at[k, w], yrs.at[k, w], across).start()

    def pair(src, k, row, zz):
        remote(src, block(k, row, zz), dss.at[k, row * 4 + zz], drs.at[k, row * 4 + zz], partner).start()

    def arrived(ref, sem):
        remote(ref, ref, sem, sem, partner).wait_recv()
        return ref

    def left(ref, sem):
        remote(ref, ref, sem, sem, partner).wait_send()

    def which(d, side):
        return 2 * d - 1 + side

    own = [s.at[layer] for s, _, layer in chunks]
    for k in [last, *range(last)]:
        over(own[k], k, z, 0)
    kept = [pltpu.make_async_copy(src, block(k, y, z), ls.at[k]) for k, src in enumerate(own)]
    for k, src in enumerate(own):
        for side in sides:
            along(src, k, z, 1, side)
        pair(src, k, y, z)
        kept[k].start()
    src = arrived(block(last, 1 - y, z), yrs.at[last, 0])
    for side in sides:
        along(src, last + 1, z, 1, side)
    pair(src, last, 1 - y, z)

    def crossed(d, k):
        for side in sides[: 1 + min(d, 1)]:

            def hand(zz, w):
                pair(arrived(block(k, 1 - y, zz), yrs.at[k, w]), k, 1 - y, zz)

            if d:
                when(there(d, side))(functools.partial(hand, at(d, side), which(d, side)))
            else:
                hand(z, 0)

    for d in (1, 2, 3):
        for e, (k, row) in enumerate(entries):
            for side in sides:

                @when(there(d, side))
                def _():
                    zz = at(d, side)
                    src = arrived(block(k, row, zz), zrs.at[e, d - 1, side])
                    if d < 3:
                        along(src, e, zz, d + 1, side)
                    if k != last:
                        over(src, k, zz, which(d, side))
                    pair(src, k, row, zz)

            if k != last:
                crossed(d - 1, k)
    for k in range(last):
        crossed(3, k)

    for k in range(last + 1):
        for b in range(8):
            left(arrived(block(k, 0, b, 1 - c), drs.at[k, b]), dss.at[k, b])
        left(own[k], yss.at[k, 0])
    for d in range(3):
        for side in sides:
            for e in range(len(entries)):
                when(goes_on[side] & there(d, side))(functools.partial(left, own[entries[e][0]], zss.at[e, d, side]))
            for k in range(last):
                when(there(d + 1, side))(functools.partial(left, own[k], yss.at[k, which(d + 1, side)]))
    finish(kept)


def all_gather(*shards):
    out = pl.pallas_call(
        gather_kernel,
        out_shape=[jax.ShapeDtypeStruct((2, 16, *s.shape[1:]), bf16) for s in shards],
        in_specs=[pl.BlockSpec(memory_space=HBM)] * 3,
        out_specs=[pl.BlockSpec(memory_space=pl.ANY)] * 3,
        scratch_shapes=[DMA((7, 3, 2)), DMA((7, 3, 2)), DMA((6, 7)), DMA((6, 7)), DMA((6, 8)), DMA((6, 8)), DMA((6,))],
        compiler_params=pltpu.CompilerParams(collective_id=1, has_side_effects=True, vmem_limit_bytes=2**23),
    )(*shards)
    return [o.reshape(2, -1, o.shape[-1]) for o in out]


def settle_kernel(*refs):
    sems = refs[-1]
    copies = [pltpu.make_async_copy(src.at[layer], dst.at[layer], sems.at[i, layer]) for i, (src, dst) in enumerate(zip(refs[:3], refs[3:6], strict=True)) for layer in range(2)]
    start(copies)
    finish(copies)


def settle(arrays):
    return pl.pallas_call(
        settle_kernel,
        out_shape=[jax.ShapeDtypeStruct(a.shape, a.dtype) for a in arrays],
        in_specs=[pl.BlockSpec(memory_space=pl.ANY)] * 3,
        out_specs=[pl.BlockSpec(memory_space=HBM)] * 3,
        scratch_shapes=[DMA((3, 2))],
        compiler_params=pltpu.CompilerParams(vmem_limit_bytes=2**20),
    )(*arrays)


def adamw(w, m, v, g):
    m = 0.9 * m + 0.1 * g
    v = 0.95 * v + 0.05 * g * g
    step = m * lax.rsqrt(v + 1e-8) + 0.1 * w
    return (w - 0.02 * step).astype(bf16), m, v


def solution(mesh):
    def step(x, dy, wg, wu, wd, mg, mu, md, vg, vu, vd):
        a0, a1, h1, p0, s0, mid0, p1, s1, mid1 = forward(x[0], wg, wu, wd)
        gg, gd, sums, _ = backward(dy[0], h1, a1, a0, p1, s1, mid1, p0, s0, mid0, wg, wu, wd)
        factor = jnp.minimum(1.0, 0.5 * lax.rsqrt(jnp.sum(sums) / (6 * D * FF) + 1e-30))
        me = lax.axis_index("dp")
        new = []
        for w, m, v, g in ((wg, mg, vg, gg[0]), (wu, mu, vu, gg[1]), (wd, md, vd, gd.reshape(2, 200, D))):
            rows = m.shape[1]
            mine = lax.dynamic_slice_in_dim(w, me * rows, rows, 1)
            new.append(adamw(mine.astype(f32), m, v, g.astype(f32) * factor))
        weights = settle(all_gather(*(n[0] for n in new)))
        return (*weights, *(n[1] for n in new), *(n[2] for n in new))

    seq, rep, own = P(("rep", "dp")), P("rep"), P("rep", "dp")
    return jax.shard_map(
        step,
        mesh=mesh,
        in_specs=(seq, seq, P(), P(), P(), *[P(None, "dp")] * 6),
        out_specs=(rep,) * 3 + (own,) * 6,
        check_vma=False,
    )
```
